256 devices in a mesh: seq: 16 (over x, z_lo), row: 2 (over core), col: 8 (over z_hi, y).
Axes of the slice: x: 4, y: 4, z: 8 (z_hi: 2, z_lo: 4; z = z_hi * 4 + z_lo), core: 2. Of those that a mesh axis runs over, the one named last changes fastest.
Arguments:
- tokens: bfloat16 [8192, 6144], P('seq', ('row', 'col')), may hold values from -20 to 20
- ln_gain: bfloat16 [6144], P(('row', 'col')), may hold values from 0.099609375 to 1.8984375
- ln_bias: bfloat16 [6144], P(('row', 'col')), may hold values from -1.5 to 1.5
- w_qkv: bfloat16 [3, 6144, 4096], P(None, 'row', 'col'), may hold values from -3 to 3
- w_out: bfloat16 [4096, 6144], P('col', 'row'), may hold values from -0.5 to 0.5
Outputs:
- attended: bfloat16 [8192, 6144], P('seq', ('row', 'col'))
The draws below stay inside these ranges and needn't reach their ends.
All inputs are finite; a program needn't handle non-finite values.
Results may differ from the reference program's by a relative error of at most 0.014.
Values may be sent and summed in bfloat16 or wider, within the bound.
A program may use at most 128 MiB of HBM per device.

```python
import math
import jax
import jax.numpy as jnp
from jax import lax

D = 6144
H = 32
HD = 128
T_SIZE = 8192


def draw_tokens(key, part):
    subkeys = jax.random.split(key, 3)
    group_size = max(D // 48, 1)
    group_count = D // group_size
    scale_levels = jnp.exp(jax.random.uniform(subkeys[0], (T_SIZE, group_count), jnp.float32, jnp.log(0.2), jnp.log(3.0)))
    scale_levels = jnp.repeat(scale_levels, group_size, axis=1)
    offsets = 0.5 * jnp.clip(jax.random.normal(subkeys[1], (T_SIZE, 1), jnp.float32), -4.0, 4.0)
    noise = jnp.clip(jax.random.normal(subkeys[2], (T_SIZE, D), jnp.float32), -4.0, 4.0)
    values = offsets + scale_levels * noise
    return values.astype(jnp.bfloat16)


def draw_w_qkv(key, part):
    subkeys = jax.random.split(key, 1)
    base = jnp.clip(jax.random.normal(subkeys[0], (3, D, H * HD), jnp.float32), -4.0, 4.0)
    factors = jnp.array([1.4, 1.4, 1.0], jnp.float32)[:, None, None] / jnp.sqrt(jnp.float32(D))
    weights = base * factors
    return weights.astype(jnp.bfloat16)


def steps_of(own_key, dims, pieces, low, high):
    level, own = 1.0, jax.random.fold_in(own_key, 6)
    for axis_at, parts in pieces:
        draws = jnp.exp(jax.random.uniform(jax.random.fold_in(own, axis_at), (parts,), jnp.float32, low / len(pieces), high / len(pieces)))
        level = level * jnp.repeat(draws, dims[axis_at] // parts).reshape([-1 if axis == axis_at else 1 for axis in range(len(dims))])
    return level


def normal_values(rng, shape, deviation, bound, cuts=(), kind=jnp.bfloat16):
    level = steps_of(rng, shape, cuts, -0.22, 0.18) if cuts else 1.0
    drawn = jax.random.normal(rng, shape, jnp.float32) * deviation * level
    return jnp.minimum(jnp.maximum(drawn, -bound), bound).astype(kind)


def setup_inputs(seed: int = 0) -> dict:
    seeds = jax.random.split(jax.random.key(seed), 6)
    tokens = draw_tokens(jax.random.fold_in(seeds[5], 71), 0)
    ln_gain = jnp.clip(1.0 + 0.18 * jax.random.normal(seeds[1], (D,), jnp.float32), 0.099609375, 1.8984375).astype(jnp.bfloat16)
    ln_bias = normal_values(seeds[2], (D,), 0.3, 1.5, ((0, 16),))
    w_qkv = draw_w_qkv(jax.random.fold_in(seeds[5], 71), 0)
    w_out = normal_values(seeds[4], (H * HD, D), HD ** -0.5, 0.5, ((0, 8), (1, 2)))
    return dict(tokens=tokens, ln_gain=ln_gain, ln_bias=ln_bias, w_qkv=w_qkv, w_out=w_out)


EPS = 0.25

def reference(tokens, ln_gain, ln_bias, w_qkv, w_out):
    as_float = tokens.astype(jnp.float32)
    token_mean = lax.optimization_barrier(jnp.sum(as_float, axis=1, keepdims=True)) / D
    meansq = lax.optimization_barrier(jnp.sum(as_float * as_float, axis=1, keepdims=True)) / D
    normed = ((as_float - token_mean) * lax.rsqrt(meansq - token_mean * token_mean + EPS) * ln_gain.astype(jnp.float32) + ln_bias.astype(jnp.float32)).astype(jnp.bfloat16)
    query_all = jnp.dot(normed, w_qkv[0], preferred_element_type=jnp.float32).astype(jnp.bfloat16)
    key_all = jnp.dot(normed, w_qkv[1], preferred_element_type=jnp.float32).astype(jnp.bfloat16)
    value_all = jnp.dot(normed, w_qkv[2], preferred_element_type=jnp.float32).astype(jnp.bfloat16)
    score_scale = 1.0 / math.sqrt(HD)

    def one_head(head_index):
        first_col = (head_index * HD).astype(jnp.int32)
        query_head = lax.dynamic_slice_in_dim(query_all, first_col, HD, 1)
        key_head = lax.dynamic_slice_in_dim(key_all, first_col, HD, 1)
        value_head = lax.dynamic_slice_in_dim(value_all, first_col, HD, 1)
        scores = jnp.dot(query_head, key_head.T, preferred_element_type=jnp.float32) * score_scale
        weights = jnp.exp(scores - lax.optimization_barrier(jnp.max(scores, axis=1, keepdims=True)))
        rowsum = lax.optimization_barrier(jnp.sum(weights, axis=1, keepdims=True))
        blended = jnp.dot(weights.astype(jnp.bfloat16), value_head, preferred_element_type=jnp.float32) / rowsum
        return blended.astype(jnp.bfloat16)
    per_head = lax.map(one_head, jnp.arange(H, dtype=jnp.int32))
    context = jnp.transpose(per_head, (1, 0, 2)).reshape(query_all.shape[0], H * HD)
    attended = as_float + jnp.dot(context, w_out, preferred_element_type=jnp.float32)
    return attended.astype(jnp.bfloat16)
```

```python
import math

import jax
import jax.numpy as jnp
from jax import lax
from jax.experimental import pallas as pl
from jax.experimental.pallas import tpu as pltpu
from jax.sharding import Mesh
from jax.sharding import PartitionSpec as P

AXES = ("x", "zl", "row", "zh", "y")
MESH = pl.DeviceIdType.MESH
F32, BF16 = jnp.float32, jnp.bfloat16
D = 6144
EPS = 0.25
HD = 128
TOK = 512
HALF = 256
FEAT = 384
GB = 16
SCALE = math.log2(math.e) / math.sqrt(HD)
QB = 256
OWN, OTHER = 0, 1
HERE, RIGHT, LEFT, OPP = 0, 1, 2, 3
N_COPIES = 90


def dot(a, b, dims=((1,), (0,))):
    return lax.dot_general(a, b, (dims, ((), ())), preferred_element_type=F32)


def kernel(
    tok_ref,
    gb_ref,
    w_ref,
    wo_ref,
    out_ref,
    slabs,
    normed,
    w_vm,
    wo_vm,
    acc,
    arrived,
    stats,
    columns,
    outgoing,
    q_vm,
    kv,
    top,
    blended,
    ctx_out,
    ctx,
    partial,
    landed,
    send_sems,
    recv_sems,
    load_sems,
):
    at = {a: lax.axis_index(a) for a in AXES}
    sizes = dict(x=4, zl=4, row=2, zh=2, y=4)

    def shifted(**by):
        return {
            a: lax.rem(at[a] + (by[a] % sizes[a]), sizes[a]) if a in by else at[a] for a in AXES
        }

    mate = shifted(row=1)
    far = shifted(zh=1)
    y_right, y_left, y_opp = shifted(y=1), shifted(y=-1), shifted(y=2)
    x_right, x_left = shifted(x=1), shifted(x=-1)
    z_fwd = [None] + [shifted(zl=d) for d in (1, 2, 3)]
    z_back = [None] + [shifted(zl=-d) for d in (1, 2, 3)]
    copies = []

    def send(src, dst, device):
        i = len(copies)
        copy = pltpu.make_async_remote_copy(
            src_ref=src,
            dst_ref=dst,
            send_sem=send_sems.at[i],
            recv_sem=recv_sems.at[i],
            device_id=device,
            device_id_type=MESH,
        )
        copy.start()
        copies.append(copy)
        return copy

    loads = []

    def load(src, dst):
        copy = pltpu.make_async_copy(src, dst, load_sems.at[len(loads)])
        copy.start()
        loads.append(copy)
        return copy

    own_tok = load(tok_ref, slabs.at[0, pl.ds(0, TOK)])
    own_gb = load(gb_ref, slabs.at[0, pl.ds(TOK, GB)])

    y_of = [at["y"], y_left["y"], y_right["y"], y_opp["y"]]
    head_of = [at["zl"]] + [z_fwd[d]["zl"] for d in (1, 2, 3)]
    w_loads = []
    for slot in range(8):
        zh = at["zh"] if slot < 4 else far["zh"]
        first = (zh * 4 + y_of[slot % 4]) * FEAT
        w_loads.append(
            [
                load(
                    w_ref.at[:, pl.ds(first, FEAT), pl.ds(head_of[d] * HD, HD)],
                    w_vm.at[slot // 2, :, pl.ds((slot % 2) * FEAT, FEAT), pl.ds(d * HD, HD)],
                )
                for d in range(4)
            ]
        )

    barrier = pltpu.get_barrier_semaphore()
    partners = [mate, far, y_right, y_left, y_opp, x_right, x_left, *z_fwd[1:]]
    for p in partners:
        pl.semaphore_signal(barrier, inc=1, device_id=p, device_id_type=MESH)
    pl.semaphore_wait(barrier, len(partners))

    chunks = (pl.ds(0, HALF), pl.ds(HALF, HALF + GB))

    def move(src_slot, dst_slot, chunk, device):
        return send(slabs.at[src_slot, chunks[chunk]], slabs.at[dst_slot, chunks[chunk]], device)

    own_tok.wait()
    own_gb.wait()
    z_in = [move(0, 4, 0, far)]
    l_in, r_in = [None, None], [None, None]
    l_in[0] = move(0, 1, 0, y_right)
    r_in[1] = move(0, 2, 1, y_left)
    z_in.append(move(0, 4, 1, far))
    l_in[1] = move(0, 1, 1, y_right)
    r_in[0] = move(0, 2, 0, y_left)

    rows8 = lax.broadcasted_iota(jnp.int32, (8, FEAT), 0)
    pick_sum = (rows8 < 4).astype(F32).astype(BF16)
    pick_sq = (rows8 >= 4).astype(F32).astype(BF16)
    mine = slabs[0, :TOK, :]
    squares = mine.astype(F32) * mine.astype(F32)
    high = squares.astype(BF16)
    low = (squares - high.astype(F32)).astype(BF16)
    wide = (
        dot(pick_sum, mine, ((1,), (1,)))
        + dot(pick_sq, high, ((1,), (1,)))
        + dot(pick_sq, low, ((1,), (1,)))
    )
    rows = lax.broadcasted_iota(jnp.int32, (8, 128), 0)
    compact = jnp.zeros((8, 128), F32)
    for j in range(4):
        compact = jnp.where(rows % 4 == j, wide[:, j * 128 : (j + 1) * 128], compact)
    stats[0] = compact
    send(stats.at[0], stats.at[1], mate).wait_recv()
    compact = compact + stats[1]
    stats[2] = compact
    send(stats.at[2], stats.at[3], far).wait_recv()

    l_in[0].wait_recv()
    o_in = [move(1, 3, 0, y_right), None]
    r_in[1].wait_recv()
    o_in[1] = move(2, 3, 1, y_left)

    compact = compact + stats[3]
    stats[4] = compact
    st = [
        send(stats.at[4], stats.at[5], y_right),
        send(stats.at[4], stats.at[6], y_left),
        send(stats.at[4], stats.at[7], y_opp),
    ]
    for s in st:
        s.wait_recv()
    compact = compact + stats[5] + stats[6] + stats[7]
    average = compact / D
    mean_below = pltpu.roll(average, 4, axis=0)
    spread = average - mean_below * mean_below
    both = jnp.where(rows < 4, average, lax.rsqrt(spread + EPS))
    columns[...] = jnp.transpose(jnp.concatenate([both] * 16, axis=0))

    def normalize(slot):
        gb = slabs[slot, TOK : TOK + GB, :].astype(F32)
        gain, bias = gb[0:1], gb[8:9]
        for j in range(4):
            x = slabs[slot, j * 128 : (j + 1) * 128, :].astype(F32)
            mean, rstd = columns[:, j : j + 1], columns[:, 4 + j : 5 + j]
            normed[j * 128 : (j + 1) * 128, (slot % 2) * FEAT : (slot % 2 + 1) * FEAT] = (
                (x - mean) * rstd * gain + bias
            ).astype(BF16)

    def project(pair, k):
        product = dot(normed[...], w_vm[pair, k])
        acc[k] = product if pair == 0 else acc[k] + product

    def weights_in(pair):
        for slot in (2 * pair, 2 * pair + 1):
            for c in w_loads[slot]:
                c.wait()

    normalize(0)
    z_in[0].wait_recv()
    zl_in, zr_in = [move(4, 5, 0, y_right), None], [move(4, 6, 0, y_left), None]
    l_in[1].wait_recv()
    normalize(1)
    weights_in(0)
    for k in range(3):
        project(0, k)
    r_in[0].wait_recv()
    normalize(2)
    o_in[0].wait_recv()
    o_in[1].wait_recv()
    normalize(3)
    weights_in(1)
    for k in range(3):
        project(1, k)

    wo_loads = []
    y_dest = [at["y"], y_right["y"], y_left["y"], y_opp["y"]]
    for b in range(8):
        zh = at["zh"] if b < 4 else far["zh"]
        first = (zh * 4 + y_dest[b % 4]) * FEAT
        for d in range(4):
            wo_loads.append(
                load(
                    wo_ref.at[pl.ds(head_of[d] * HD, HD), pl.ds(first, FEAT)],
                    wo_vm.at[b, pl.ds(d * HD, HD)],
                )
            )

    zl_in[0].wait_recv()
    zo_in = [move(5, 7, 0, y_right), None]
    z_in[1].wait_recv()
    zr_in[1] = move(4, 6, 1, y_left)
    zl_in[1] = move(4, 5, 1, y_right)
    normalize(4)
    zr_in[1].wait_recv()
    zo_in[1] = move(6, 7, 1, y_left)
    zl_in[1].wait_recv()
    normalize(5)
    weights_in(2)
    for k in range(3):
        project(2, k)
    zr_in[0].wait_recv()
    normalize(6)
    zo_in[0].wait_recv()
    zo_in[1].wait_recv()
    normalize(7)
    weights_in(3)

    keep = pl.ds(at["row"] * HALF, HALF)
    give = pl.ds(mate["row"] * HALF, HALF)
    halves = {}
    for k in (1, 2, 0):
        project(3, k)
        halves[k] = send(acc.at[k, give], arrived.at[k], mate)
    z_sent = {}
    for k in (1, 2, 0):
        halves[k].wait_recv()
        whole = acc[k, keep, :] + arrived[k]
        if k == 0:
            whole = whole * SCALE
        whole = whole.astype(BF16)
        for d in (1, 2, 3):
            outgoing[k, d - 1] = whole[:, d * HD : (d + 1) * HD]
            target = q_vm.at[d] if k == 0 else kv.at[0, 0, k - 1, d]
            z_sent[k, d] = send(outgoing.at[k, d - 1], target, z_fwd[d])
        if k == 0:
            q_vm[0] = whole[:, :HD]
        else:
            kv[0, 0, k - 1, 0] = whole[:, :HD]

    right_in, left_in, opp_in, mate_in = {}, {}, {}, {}

    def to_mate(side, d):
        mate_in[side, d] = send(kv.at[side, 0, :, d], kv.at[side, 1, :, d], mate)

    def spread_own(d):
        left_in[d] = send(kv.at[0, 0, :, d], kv.at[1, 0, :, d], x_right)
        right_in[d] = send(kv.at[0, 0, :, d], kv.at[2, 0, :, d], x_left)
        to_mate(0, d)

    def pass_on(d):
        left_in[d].wait_recv()
        if d < 2:
            opp_in[d] = send(kv.at[1, 0, :, d], kv.at[3, 0, :, d], x_right)
        to_mate(1, d)
        right_in[d].wait_recv()
        if d >= 2:
            opp_in[d] = send(kv.at[2, 0, :, d], kv.at[3, 0, :, d], x_left)
        to_mate(2, d)

    spread_own(0)
    for d in (1, 2, 3):
        z_sent[1, d].wait_recv()
        z_sent[2, d].wait_recv()
        spread_own(d)
        if d >= 2:
            pass_on(d - 2)
    for d in (1, 2, 3):
        z_sent[0, d].wait_recv()

    per_slot = 4 * HALF
    n_q = per_slot // QB
    ones = jnp.ones((per_slot, HD), BF16)

    def attend(side, core, first):
        def block(i, carry):
            at_q = pl.ds(pl.multiple_of(i * QB, QB), QB)
            q = q_vm[...].reshape(per_slot, HD) if n_q == 1 else q_vm[i]
            keys = kv[side, core, 0].reshape(per_slot, HD)
            values = kv[side, core, 1].reshape(per_slot, HD)
            scores = dot(q, keys, ((1,), (1,)))
            best = jnp.max(scores, axis=1, keepdims=True)
            if not first:
                before = top[at_q, 0:1]
                best = jnp.maximum(before, best)
            weights = jnp.exp2(scores - best).astype(BF16)
            product = dot(weights, jnp.concatenate([values, ones], axis=1))
            if first:
                blended[at_q, :] = product
            else:
                blended[at_q, :] = blended[at_q, :] * jnp.exp2(before - best) + product
            top[at_q, :] = jnp.broadcast_to(best, (QB, 128))
            return carry

        lax.fori_loop(0, n_q, block, 0)

    attend(0, 0, True)
    for d in range(4):
        mate_in[0, d].wait_recv()
    pass_on(2)
    attend(0, 1, False)
    pass_on(3)
    attend(1, 0, False)
    attend(2, 0, False)
    for side in (1, 2):
        for d in range(4):
            mate_in[side, d].wait_recv()
    for d in range(4):
        opp_in[d].wait_recv()
        to_mate(3, d)
    attend(1, 1, False)
    attend(2, 1, False)
    attend(3, 0, False)
    for d in range(4):
        mate_in[3, d].wait_recv()
    attend(3, 1, False)

    c_in = {}
    for d in (1, 2, 3, 0):
        rows_d = slice(d * HALF, (d + 1) * HALF)
        value = (blended[rows_d, :HD] / blended[rows_d, HD:]).astype(BF16)
        if d == 0:
            ctx[0, 0] = value
        else:
            ctx_out[d - 1] = value
            c_in[d] = send(ctx_out.at[d - 1], ctx.at[0, d], z_back[d])
    m_in = [send(ctx.at[0, 0], ctx.at[1, 0], mate)]
    for d in (1, 2, 3):
        c_in[d].wait_recv()
        m_in.append(send(ctx.at[0, d], ctx.at[1, d], mate))
    for c in wo_loads:
        c.wait()

    def product(z, y, j):
        a = jnp.concatenate([ctx[j, d] for d in range(4)], axis=1)
        return dot(a, wo_vm[4 * z + y])

    out_in = {}
    names = {}

    def push(name, j, value, device):
        n = names.setdefault(name, len(names))
        partial[n, j] = value.astype(BF16)
        out_in[name, j] = send(partial.at[n, j], landed.at[n, j], device)

    def got(name, j):
        out_in[name, j].wait_recv()
        return landed[names[name], j].astype(F32)

    for j in (0, 1):
        if j == 1:
            for m in m_in:
                m.wait_recv()
        push("o_opp", j, product(OTHER, OPP, j), y_right)
        push("o_right", j, product(OTHER, LEFT, j), y_left)
    for j in (0, 1):
        push("w_opp", j, product(OWN, OPP, j), y_left)
    for j in (0, 1):
        push("o_left", j, product(OTHER, RIGHT, j) + got("o_opp", j), y_right)
    for j in (0, 1):
        push("w_left", j, product(OWN, RIGHT, j), y_right)
    for j in (0, 1):
        push("w_right", j, product(OWN, LEFT, j) + got("w_opp", j), y_left)
        push("z", j, product(OTHER, HERE, j) + got("o_left", j) + got("o_right", j), far)
    for j in (0, 1):
        rows_j = keep if j == 0 else give
        total = product(OWN, HERE, j) + got("w_left", j) + got("w_right", j)
        total = total + got("z", j) + slabs[0, rows_j, :].astype(F32)
        out_ref[rows_j, :] = total.astype(BF16)
    for copy in copies:
        copy.wait_send()


def body(tokens, ln_gain, ln_bias, w_qkv, w_out):
    gb = jnp.concatenate(
        [jnp.broadcast_to(ln_gain[None], (8, FEAT)), jnp.broadcast_to(ln_bias[None], (8, FEAT))]
    )
    any_spec = pl.BlockSpec(memory_space=pl.ANY)
    return pl.pallas_call(
        kernel,
        out_shape=jax.ShapeDtypeStruct((TOK, FEAT), BF16),
        in_specs=[any_spec] * 4,
        out_specs=pl.BlockSpec(memory_space=pltpu.VMEM),
        scratch_shapes=[
            pltpu.VMEM((8, TOK + GB, FEAT), BF16),
            pltpu.VMEM((TOK, 2 * FEAT), BF16),
            pltpu.VMEM((4, 3, 2 * FEAT, 4 * HD), BF16),
            pltpu.VMEM((8, 4 * HD, FEAT), BF16),
            pltpu.VMEM((3, TOK, 4 * HD), F32),
            pltpu.VMEM((3, HALF, 4 * HD), F32),
            pltpu.VMEM((8, 8, 128), F32),
            pltpu.VMEM((128, 128), F32),
            pltpu.VMEM((3, 3, HALF, HD), BF16),
            pltpu.VMEM((4, HALF, HD), BF16),
            pltpu.VMEM((4, 2, 2, 4, HALF, HD), BF16),
            pltpu.VMEM((4 * HALF, 128), F32),
            pltpu.VMEM((4 * HALF, 2 * HD), F32),
            pltpu.VMEM((3, HALF, HD), BF16),
            pltpu.VMEM((2, 4, HALF, HD), BF16),
            pltpu.VMEM((7, 2, HALF, FEAT), BF16),
            pltpu.VMEM((7, 2, HALF, FEAT), BF16),
            pltpu.SemaphoreType.DMA((N_COPIES,)),
            pltpu.SemaphoreType.DMA((N_COPIES,)),
            pltpu.SemaphoreType.DMA((66,)),
        ],
        compiler_params=pltpu.CompilerParams(
            collective_id=0, has_side_effects=True, vmem_limit_bytes=60 * 2**20
        ),
    )(tokens, gb, w_qkv, w_out)


def solution(mesh):
    finer = Mesh(mesh.devices.reshape(4, 4, 2, 2, 4), AXES)
    seq, row_col, col = ("x", "zl"), ("row", "zh", "y"), ("zh", "y")
    in_specs = (P(seq, row_col), P(row_col), P(row_col), P(None, "row", col), P(col, "row"))
    return jax.shard_map(
        body, mesh=finer, in_specs=in_specs, out_specs=P(seq, row_col), check_vma=False
    )
```

```python
import math

import jax
import jax.numpy as jnp
from jax import lax
from jax.experimental import pallas as pl
from jax.experimental.pallas import tpu as pltpu
from jax.sharding import Mesh
from jax.sharding import PartitionSpec as P

AXES = ("x", "zl", "row", "zh", "y")
MESH = pl.DeviceIdType.MESH
F32, BF16 = jnp.float32, jnp.bfloat16
D = 6144
EPS = 0.25
HD = 128
TOK = 512
QUARTER = 128
HALF = 256
FEAT = 384
GB = 16
SCALE = math.log2(math.e) / math.sqrt(HD)
KEYS = 512
OWN, OTHER = 0, 1
HERE, RIGHT, LEFT, OPP = 0, 1, 2, 3
N_COPIES = 140


def dot(a, b, dims=((1,), (0,))):
    return lax.dot_general(a, b, (dims, ((), ())), preferred_element_type=F32)


def kernel(
    tok_ref,
    gb_ref,
    w_ref,
    wo_ref,
    out_ref,
    slabs,
    normed,
    w_vm,
    wo_vm,
    acc,
    arrived,
    stats,
    columns,
    outgoing,
    q_vm,
    kv,
    top,
    blended,
    ctx_out,
    ctx,
    partial,
    landed,
    send_sems,
    recv_sems,
    load_sems,
):
    at = {a: lax.axis_index(a) for a in AXES}
    sizes = dict(x=4, zl=4, row=2, zh=2, y=4)

    def shifted(**by):
        return {
            a: lax.rem(at[a] + (by[a] % sizes[a]), sizes[a]) if a in by else at[a] for a in AXES
        }

    mate = shifted(row=1)
    far = shifted(zh=1)
    far_mate = shifted(zh=1, row=1)
    y_right, y_left, y_opp = shifted(y=1), shifted(y=-1), shifted(y=2)
    x_right, x_left = shifted(x=1), shifted(x=-1)
    z_fwd = [None] + [shifted(zl=d) for d in (1, 2, 3)]
    z_back = [None] + [shifted(zl=-d) for d in (1, 2, 3)]
    copies = []

    def send(src, dst, device):
        i = len(copies)
        copy = pltpu.make_async_remote_copy(
            src_ref=src,
            dst_ref=dst,
            send_sem=send_sems.at[i],
            recv_sem=recv_sems.at[i],
            device_id=device,
            device_id_type=MESH,
        )
        copy.start()
        copies.append(copy)
        return copy

    loads = []

    def load(src, dst):
        copy = pltpu.make_async_copy(src, dst, load_sems.at[len(loads)])
        copy.start()
        loads.append(copy)
        return copy

    own_tok = load(tok_ref, slabs.at[0, pl.ds(GB, TOK)])
    own_gb = load(gb_ref, slabs.at[0, pl.ds(0, GB)])

    y_of = [at["y"], y_left["y"], y_right["y"], y_opp["y"]]
    head_of = [at["zl"]] + [z_fwd[d]["zl"] for d in (1, 2, 3)]
    w_loads = []
    for slot in range(8):
        zh = at["zh"] if slot < 4 else far["zh"]
        first = (zh * 4 + y_of[slot % 4]) * FEAT
        w_loads.append(
            [
                load(
                    w_ref.at[:, pl.ds(first, FEAT), pl.ds(head_of[d] * HD, HD)],
                    w_vm.at[slot // 2, :, pl.ds((slot % 2) * FEAT, FEAT), pl.ds(d * HD, HD)],
                )
                for d in range(4)
            ]
        )

    barrier = pltpu.get_barrier_semaphore()
    partners = [mate, far, far_mate, y_right, y_left, y_opp, x_right, x_left, *z_fwd[1:]]
    for p in partners:
        pl.semaphore_signal(barrier, inc=1, device_id=p, device_id_type=MESH)
    own_tok.wait()
    own_gb.wait()

    rows8 = lax.broadcasted_iota(jnp.int32, (8, FEAT), 0)
    pick_sum = (rows8 < 4).astype(F32).astype(BF16)
    pick_sq = (rows8 >= 4).astype(F32).astype(BF16)
    mine = slabs[0, GB:, :]
    squares = mine.astype(F32) * mine.astype(F32)
    high = squares.astype(BF16)
    low = (squares - high.astype(F32)).astype(BF16)
    wide = (
        dot(pick_sum, mine, ((1,), (1,)))
        + dot(pick_sq, high, ((1,), (1,)))
        + dot(pick_sq, low, ((1,), (1,)))
    )
    rows = lax.broadcasted_iota(jnp.int32, (8, 128), 0)
    compact = jnp.zeros((8, 128), F32)
    for j in range(4):
        compact = jnp.where(rows % 4 == j, wide[:, j * 128 : (j + 1) * 128], compact)
    stats[0] = compact
    pl.semaphore_wait(barrier, len(partners))
    st = [
        send(stats.at[0], stats.at[1], mate),
        send(stats.at[0], stats.at[2], far),
        send(stats.at[0], stats.at[3], far_mate),
    ]

    chunks = [pl.ds(0, GB + QUARTER)] + [pl.ds(GB + i * QUARTER, QUARTER) for i in (1, 2, 3)]

    def move(src_slot, dst_slot, chunk, device):
        return send(slabs.at[src_slot, chunks[chunk]], slabs.at[dst_slot, chunks[chunk]], device)

    from_left, from_right, from_opp = [{}, {}], [{}, {}], [{}, {}]

    def offer(z, i):
        from_left[z][i] = move(4 * z, 4 * z + 1, i, y_right)
        from_right[z][i] = move(4 * z, 4 * z + 2, i, y_left)

    def relay(z, i):
        if i % 2 == 0:
            from_left[z][i].wait_recv()
            from_opp[z][i] = move(4 * z + 1, 4 * z + 3, i, y_right)
        else:
            from_right[z][i].wait_recv()
            from_opp[z][i] = move(4 * z + 2, 4 * z + 3, i, y_left)

    z_in = []
    for i in range(4):
        z_in.append(move(0, 4, i, far))
        offer(OWN, i)

    def offer_far(i):
        z_in[i].wait_recv()
        offer(OTHER, i)

    for s in st:
        s.wait_recv()
    compact = compact + stats[1] + stats[2] + stats[3]
    stats[4] = compact
    st = [
        send(stats.at[4], stats.at[5], y_right),
        send(stats.at[4], stats.at[6], y_left),
        send(stats.at[4], stats.at[7], y_opp),
    ]
    relay(OWN, 0)
    relay(OWN, 1)
    offer_far(0)
    relay(OWN, 2)
    relay(OWN, 3)
    for s in st:
        s.wait_recv()
    compact = compact + stats[5] + stats[6] + stats[7]
    average = compact / D
    mean_below = pltpu.roll(average, 4, axis=0)
    spread = average - mean_below * mean_below
    both = jnp.where(rows < 4, average, lax.rsqrt(spread + EPS))
    columns[...] = jnp.transpose(jnp.concatenate([both] * 16, axis=0))

    def normalize(slot, groups=range(4)):
        gb = slabs[slot, :GB, :].astype(F32)
        gain, bias = gb[0:1], gb[8:9]
        for j in groups:
            x = slabs[slot, GB + j * 128 : GB + (j + 1) * 128, :].astype(F32)
            mean, rstd = columns[:, j : j + 1], columns[:, 4 + j : 5 + j]
            normed[j * 128 : (j + 1) * 128, (slot % 2) * FEAT : (slot % 2 + 1) * FEAT] = (
                (x - mean) * rstd * gain + bias
            ).astype(BF16)

    def project(pair, k, rows=slice(0, TOK)):
        product = dot(normed[rows], w_vm[pair, k])
        acc[k, rows] = product if pair == 0 else acc[k, rows] + product

    def weights_in(pair):
        for slot in (2 * pair, 2 * pair + 1):
            for c in w_loads[slot]:
                c.wait()

    normalize(0)
    offer_far(1)
    for i in (1, 3):
        from_left[OWN][i].wait_recv()
    normalize(1)
    weights_in(0)
    for k in range(3):
        project(0, k)
    offer_far(2)
    relay(OTHER, 0)
    for i in (0, 2):
        from_right[OWN][i].wait_recv()
    normalize(2)
    for i in range(4):
        from_opp[OWN][i].wait_recv()
    normalize(3)
    relay(OTHER, 1)
    weights_in(1)
    for k in range(3):
        project(1, k)

    wo_loads = []
    y_dest = [at["y"], y_right["y"], y_left["y"], y_opp["y"]]
    for b in range(8):
        zh = at["zh"] if b < 4 else far["zh"]
        first = (zh * 4 + y_dest[b % 4]) * FEAT
        for d in range(4):
            wo_loads.append(
                load(
                    wo_ref.at[pl.ds(head_of[d] * HD, HD), pl.ds(first, FEAT)],
                    wo_vm.at[b, pl.ds(d * HD, HD)],
                )
            )

    offer_far(3)
    relay(OTHER, 2)
    normalize(4)
    relay(OTHER, 3)
    for i in (1, 3):
        from_left[OTHER][i].wait_recv()
    normalize(5)
    weights_in(2)
    for k in range(3):
        project(2, k)
    for i in (0, 2):
        from_right[OTHER][i].wait_recv()
    normalize(6)
    weights_in(3)

    def kv_part(side, core, d, p):
        return kv.at[side, core, :, d, pl.ds(p * QUARTER, QUARTER)]

    z_kv, z_q = {}, {}
    right_in, left_in, opp_in, mate_in = {}, {}, {}, {}

    def to_mate(side, d, p):
        mate_in[side, d, p] = send(kv_part(side, 0, d, p), kv_part(side, 1, d, p), mate)

    def spread_own(d, p):
        left_in[d, p] = send(kv_part(0, 0, d, p), kv_part(1, 0, d, p), x_right)
        right_in[d, p] = send(kv_part(0, 0, d, p), kv_part(2, 0, d, p), x_left)
        to_mate(0, d, p)

    def pass_on(d, p):
        left_in[d, p].wait_recv()
        if (d + p) % 2 == 0:
            opp_in[d, p] = send(kv_part(1, 0, d, p), kv_part(3, 0, d, p), x_right)
        to_mate(1, d, p)
        right_in[d, p].wait_recv()
        if (d + p) % 2 == 1:
            opp_in[d, p] = send(kv_part(2, 0, d, p), kv_part(3, 0, d, p), x_left)
        to_mate(2, d, p)

    def z_arrived(d, p):
        z_kv[d, p].wait_recv()
        spread_own(d, p)

    for p in (0, 1):
        for i in (2 * p, 2 * p + 1):
            from_opp[OTHER][i].wait_recv()
        normalize(7, (2 * p, 2 * p + 1))
        keep_p = pl.ds(p * HALF + at["row"] * QUARTER, QUARTER)
        give_p = pl.ds(p * HALF + mate["row"] * QUARTER, QUARTER)
        rows_p = pl.ds(p * QUARTER, QUARTER)
        halves = {}
        for k in (1, 2, 0):
            project(3, k, slice(p * HALF, (p + 1) * HALF))
            halves[k] = send(acc.at[k, give_p], arrived.at[p, k], mate)
        for k in (1, 2, 0):
            halves[k].wait_recv()
            whole = acc[k, keep_p, :] + arrived[p, k]
            if k == 0:
                whole = whole * SCALE
            whole = whole.astype(BF16)
            for d in (1, 2, 3):
                outgoing[p, d - 1, k] = whole[:, d * HD : (d + 1) * HD]
            if k == 0:
                q_vm[0, rows_p] = whole[:, :HD]
                for d in (1, 2, 3):
                    z_q[d, p] = send(outgoing.at[p, d - 1, 0], q_vm.at[d, rows_p], z_fwd[d])
            else:
                kv[0, 0, k - 1, 0, rows_p] = whole[:, :HD]
            if k == 2:
                for d in (1, 2, 3):
                    z_kv[d, p] = send(
                        outgoing.at[p, d - 1, pl.ds(1, 2)], kv_part(0, 0, d, p), z_fwd[d]
                    )
                spread_own(0, p)

    z_arrived(1, 0)
    z_arrived(2, 0)
    pass_on(0, 0)
    z_arrived(3, 0)
    pass_on(0, 1)
    z_arrived(1, 1)
    pass_on(1, 0)
    z_arrived(2, 1)
    pass_on(2, 0)
    z_arrived(3, 1)
    pass_on(3, 0)
    for p in (0, 1):
        for d in (1, 2, 3):
            z_q[d, p].wait_recv()

    ones = jnp.ones((KEYS, HD), BF16)
    n_q = 4 * HALF

    def attend(slots, begin, size, first):
        at_q = pl.ds(begin, size)
        q = q_vm[begin // HALF : (begin + size) // HALF].reshape(size, HD)
        best = None if first else top[at_q, :]
        total = None if first else blended[at_q, :]
        steps = [(slot, i) for slot in slots for i in range(n_q // KEYS)]
        d_step = KEYS // HALF

        def piece(step, k):
            (side, core), i = step
            return kv[side, core, k, i * d_step : (i + 1) * d_step].reshape(KEYS, HD)

        def lanes(values):
            return [values[:, c : c + HD] for c in range(0, values.shape[1], HD)]

        scores = dot(q, piece(steps[0], 0), ((1,), (1,)))
        for n, step in enumerate(steps):
            following = None
            if n + 1 < len(steps):
                following = dot(q, piece(steps[n + 1], 0), ((1,), (1,)))
            parts = lanes(scores)
            high = parts[0]
            for part in parts[1:]:
                high = jnp.maximum(high, part)
            now = jnp.broadcast_to(jnp.max(high, axis=1, keepdims=True), (size, HD))
            if best is not None:
                now = jnp.maximum(best, now)
            weights = [jnp.exp2(part - now).astype(BF16) for part in parts]
            product = dot(
                jnp.concatenate(weights, axis=1),
                jnp.concatenate([piece(step, 1), ones], axis=1),
            )
            if best is None:
                total = product
            else:
                shrink = jnp.exp2(best - now)
                total = jnp.concatenate([part * shrink for part in lanes(total)], axis=1) + product
            best, scores = now, following
        blended[at_q, :] = total
        top[at_q, :] = best

    def mates_in(side):
        for d in range(4):
            for p in (0, 1):
                mate_in[side, d, p].wait_recv()

    attend([(0, 0)], 0, n_q, True)
    pass_on(1, 1)
    pass_on(2, 1)
    mates_in(0)
    attend([(0, 1)], 0, n_q, False)
    pass_on(3, 1)
    attend([(1, 0), (2, 0)], 0, n_q, False)
    for d in range(4):
        for p in (0, 1):
            opp_in[d, p].wait_recv()
            to_mate(3, d, p)
    for side in (1, 2, 3):
        mates_in(side)

    c_in = {}
    for begin in (2 * HALF, 0):
        attend([(1, 1), (2, 1), (3, 0), (3, 1)], begin, 2 * HALF, False)
        for d in (begin // HALF + 1, begin // HALF):
            rows_d = slice(d * HALF, (d + 1) * HALF)
            value = (blended[rows_d, :HD] / blended[rows_d, HD:]).astype(BF16)
            if d == 0:
                ctx[0, 0] = value
            else:
                ctx_out[d - 1] = value
                c_in[d] = send(ctx_out.at[d - 1], ctx.at[0, d], z_back[d])
    m_in = [send(ctx.at[0, 0], ctx.at[1, 0], mate)]
    for d in (3, 2, 1):
        c_in[d].wait_recv()
        m_in.append(send(ctx.at[0, d], ctx.at[1, d], mate))
    for c in wo_loads:
        c.wait()

    def product(z, y, j):
        a = jnp.concatenate([ctx[j, d] for d in range(4)], axis=1)
        return dot(a, wo_vm[4 * z + y])

    out_in = {}
    names = {}

    def push(name, j, value, device):
        n = names.setdefault(name, len(names))
        partial[n, j] = value.astype(BF16)
        out_in[name, j] = send(partial.at[n, j], landed.at[n, j], device)

    def got(name, j):
        out_in[name, j].wait_recv()
        return landed[names[name], j].astype(F32)

    for j in (0, 1):
        if j == 1:
            for m in m_in:
                m.wait_recv()
        push("o_opp", j, product(OTHER, OPP, j), y_right)
        push("o_right", j, product(OTHER, LEFT, j), y_left)
    for j in (0, 1):
        push("w_opp", j, product(OWN, OPP, j), y_left)
    for j in (0, 1):
        push("o_left", j, product(OTHER, RIGHT, j) + got("o_opp", j), y_right)
    for j in (0, 1):
        push("w_left", j, product(OWN, RIGHT, j), y_right)
    for j in (0, 1):
        push("w_right", j, product(OWN, LEFT, j) + got("w_opp", j), y_left)
        push("z", j, product(OTHER, HERE, j) + got("o_left", j) + got("o_right", j), far)
    for j in (0, 1):
        total = product(OWN, HERE, j) + got("w_left", j) + got("w_right", j) + got("z", j)
        core = at["row"] if j == 0 else mate["row"]
        for p in (0, 1):
            first = p * HALF + core * QUARTER
            piece = total[p * QUARTER : (p + 1) * QUARTER]
            own = slabs[0, pl.ds(GB + first, QUARTER), :].astype(F32)
            out_ref[pl.ds(first, QUARTER), :] = (piece + own).astype(BF16)
    for copy in copies:
        copy.wait_send()


def body(tokens, ln_gain, ln_bias, w_qkv, w_out):
    gb = jnp.concatenate(
        [jnp.broadcast_to(ln_gain[None], (8, FEAT)), jnp.broadcast_to(ln_bias[None], (8, FEAT))]
    )
    any_spec = pl.BlockSpec(memory_space=pl.ANY)
    return pl.pallas_call(
        kernel,
        out_shape=jax.ShapeDtypeStruct((TOK, FEAT), BF16),
        in_specs=[any_spec] * 4,
        out_specs=pl.BlockSpec(memory_space=pltpu.VMEM),
        scratch_shapes=[
            pltpu.VMEM((8, TOK + GB, FEAT), BF16),
            pltpu.VMEM((TOK, 2 * FEAT), BF16),
            pltpu.VMEM((4, 3, 2 * FEAT, 4 * HD), BF16),
            pltpu.VMEM((8, 4 * HD, FEAT), BF16),
            pltpu.VMEM((3, TOK, 4 * HD), F32),
            pltpu.VMEM((2, 3, QUARTER, 4 * HD), F32),
            pltpu.VMEM((8, 8, 128), F32),
            pltpu.VMEM((128, 128), F32),
            pltpu.VMEM((2, 3, 3, QUARTER, HD), BF16),
            pltpu.VMEM((4, HALF, HD), BF16),
            pltpu.VMEM((4, 2, 2, 4, HALF, HD), BF16),
            pltpu.VMEM((4 * HALF, 128), F32),
            pltpu.VMEM((4 * HALF, 2 * HD), F32),
            pltpu.VMEM((3, HALF, HD), BF16),
            pltpu.VMEM((2, 4, HALF, HD), BF16),
            pltpu.VMEM((7, 2, HALF, FEAT), BF16),
            pltpu.VMEM((7, 2, HALF, FEAT), BF16),
            pltpu.SemaphoreType.DMA((N_COPIES,)),
            pltpu.SemaphoreType.DMA((N_COPIES,)),
            pltpu.SemaphoreType.DMA((66,)),
        ],
        compiler_params=pltpu.CompilerParams(
            collective_id=0, has_side_effects=True, vmem_limit_bytes=60 * 2**20
        ),
    )(tokens, gb, w_qkv, w_out)


def solution(mesh):
    finer = Mesh(mesh.devices.reshape(4, 4, 2, 2, 4), AXES)
    seq, row_col, col = ("x", "zl"), ("row", "zh", "y"), ("zh", "y")
    in_specs = (P(seq, row_col), P(row_col), P(row_col), P(None, "row", col), P(col, "row"))
    return jax.shard_map(
        body, mesh=finer, in_specs=in_specs, out_specs=P(seq, row_col), check_vma=False
    )
```

```python
import math

import jax
import jax.numpy as jnp
from jax import lax
from jax.experimental import pallas as pl
from jax.experimental.pallas import tpu as pltpu
from jax.sharding import Mesh
from jax.sharding import PartitionSpec as P

AXES = ("x", "zl", "row", "zh", "y")
MESH = pl.DeviceIdType.MESH
F32, BF16 = jnp.float32, jnp.bfloat16
D = 6144
EPS = 0.25
HD = 128
TOK = 512
QUARTER = 128
HALF = 256
FEAT = 384
GB = 16
SCALE = math.log2(math.e) / math.sqrt(HD)
KEYS = 512
OWN, OTHER = 0, 1
HERE, RIGHT, LEFT, OPP = 0, 1, 2, 3
N_COPIES = 140


def dot(a, b, dims=((1,), (0,))):
    return lax.dot_general(a, b, (dims, ((), ())), preferred_element_type=F32)


def kernel(
    tok_ref,
    gain_ref,
    bias_ref,
    w_ref,
    wo_ref,
    out_ref,
    slabs,
    normed,
    w_vm,
    wo_vm,
    wo_far,
    acc,
    arrived,
    stats,
    columns,
    outgoing,
    q_vm,
    kv,
    top,
    blended,
    ctx_out,
    ctx,
    partial,
    landed,
    send_sems,
    recv_sems,
    load_sems,
    chain_send,
    chain_recv,
):
    at = {a: lax.axis_index(a) for a in AXES}
    sizes = dict(x=4, zl=4, row=2, zh=2, y=4)

    def shifted(**by):
        return {
            a: lax.rem(at[a] + (by[a] % sizes[a]), sizes[a]) if a in by else at[a] for a in AXES
        }

    mate = shifted(row=1)
    far = shifted(zh=1)
    far_mate = shifted(zh=1, row=1)
    y_right, y_left, y_opp = shifted(y=1), shifted(y=-1), shifted(y=2)
    x_right, x_left = shifted(x=1), shifted(x=-1)
    z_fwd = [None] + [shifted(zl=d) for d in (1, 2, 3)]
    z_back = [None] + [shifted(zl=-d) for d in (1, 2, 3)]
    far_back = [shifted(zh=1, zl=-d) for d in range(4)]
    z_prev = dict(at, zl=z_back[1]["zl"], zh=jnp.where(at["zl"] == 0, far["zh"], at["zh"]))
    z_next = dict(at, zl=z_fwd[1]["zl"], zh=jnp.where(at["zl"] == 3, far["zh"], at["zh"]))
    copies = []

    def send(src, dst, device):
        i = len(copies)
        copy = pltpu.make_async_remote_copy(
            src_ref=src,
            dst_ref=dst,
            send_sem=send_sems.at[i],
            recv_sem=recv_sems.at[i],
            device_id=device,
            device_id_type=MESH,
        )
        copy.start()
        copies.append(copy)
        return copy

    loads = []

    def load(src, dst):
        copy = pltpu.make_async_copy(src, dst, load_sems.at[len(loads)])
        copy.start()
        loads.append(copy)
        return copy

    own_tok = load(tok_ref, slabs.at[0, pl.ds(GB, TOK)])
    slabs[0, :GB, :] = jnp.where(
        lax.broadcasted_iota(jnp.int32, (GB, FEAT), 0) < 8,
        jnp.broadcast_to(gain_ref[...].astype(F32), (GB, FEAT)),
        jnp.broadcast_to(bias_ref[...].astype(F32), (GB, FEAT)),
    ).astype(BF16)

    y_of = [at["y"], y_left["y"], y_right["y"], y_opp["y"]]
    head_of = [at["zl"]] + [z_fwd[d]["zl"] for d in (1, 2, 3)]
    w_loads = []
    for slot in range(8):
        zh = at["zh"] if slot < 4 else far["zh"]
        first = (zh * 4 + y_of[slot % 4]) * FEAT
        w_loads.append(
            [
                load(
                    w_ref.at[:, pl.ds(first, FEAT), pl.ds(head_of[d] * HD, HD)],
                    w_vm.at[slot // 2, :, pl.ds((slot % 2) * FEAT, FEAT), pl.ds(d * HD, HD)],
                )
                for d in range(4)
            ]
        )

    barrier = pltpu.get_barrier_semaphore()
    partners = [mate, far, far_mate, y_right, y_left, y_opp, x_right, x_left, *z_fwd[1:], *far_back[1:]]
    for p in partners:
        pl.semaphore_signal(barrier, inc=1, device_id=p, device_id_type=MESH)
    own_tok.wait()

    rows8 = lax.broadcasted_iota(jnp.int32, (8, FEAT), 0)
    pick_sum = (rows8 < 4).astype(F32).astype(BF16)
    pick_sq = (rows8 >= 4).astype(F32).astype(BF16)
    mine = slabs[0, GB:, :]
    squares = mine.astype(F32) * mine.astype(F32)
    high = squares.astype(BF16)
    low = (squares - high.astype(F32)).astype(BF16)
    wide = (
        dot(pick_sum, mine, ((1,), (1,)))
        + dot(pick_sq, high, ((1,), (1,)))
        + dot(pick_sq, low, ((1,), (1,)))
    )
    rows = lax.broadcasted_iota(jnp.int32, (8, 128), 0)
    compact = jnp.zeros((8, 128), F32)
    for j in range(4):
        compact = jnp.where(rows % 4 == j, wide[:, j * 128 : (j + 1) * 128], compact)
    stats[0] = compact
    pl.semaphore_wait(barrier, len(partners))
    st = [
        send(stats.at[0], stats.at[1], mate),
        send(stats.at[0], stats.at[2], far),
        send(stats.at[0], stats.at[3], far_mate),
    ]

    chunks = [pl.ds(0, GB + QUARTER)] + [pl.ds(GB + i * QUARTER, QUARTER) for i in (1, 2, 3)]

    def move(src_slot, dst_slot, chunk, device):
        return send(slabs.at[src_slot, chunks[chunk]], slabs.at[dst_slot, chunks[chunk]], device)

    from_left, from_right, from_opp = [{}, {}], [{}, {}], [{}, {}]

    def offer(z, i):
        from_left[z][i] = move(4 * z, 4 * z + 1, i, y_right)
        from_right[z][i] = move(4 * z, 4 * z + 2, i, y_left)

    def relay(z, i):
        if i % 2 == 0:
            from_left[z][i].wait_recv()
            from_opp[z][i] = move(4 * z + 1, 4 * z + 3, i, y_right)
        else:
            from_right[z][i].wait_recv()
            from_opp[z][i] = move(4 * z + 2, 4 * z + 3, i, y_left)

    z_in = []
    for i in range(4):
        z_in.append(move(0, 4, i, far))
        offer(OWN, i)

    def offer_far(i):
        z_in[i].wait_recv()
        offer(OTHER, i)

    def hop(way, c):
        return pltpu.make_async_remote_copy(
            src_ref=wo_far.at[8 * way + 2 * at["x"] + c],
            dst_ref=wo_far.at[8 * way + 2 * at["x"] + c],
            send_sem=chain_send.at[way, c],
            recv_sem=chain_recv.at[way, c],
            device_id=z_next if way else z_prev,
            device_id_type=MESH,
        )

    place = [lax.rem(4 - at["zl"], 4), lax.rem(at["zl"] + 1, 4)]

    def chain(k):
        for way in (0, 1):
            if k < 2:

                @pl.when(place[way] == 0)
                def _():
                    block = 8 * way + 2 * at["x"] + k
                    first = (far["zh"] * 4 + lax.div(block, 4)) * FEAT
                    pltpu.make_async_remote_copy(
                        src_ref=wo_ref.at[pl.ds(lax.rem(block, 4) * HD, HD), pl.ds(first, FEAT)],
                        dst_ref=wo_far.at[block],
                        send_sem=chain_send.at[way, k],
                        recv_sem=chain_recv.at[way, k],
                        device_id=z_next if way else z_prev,
                        device_id_type=MESH,
                    ).start()

            for n in (1, 2, 3):
                c = k - 2 * n
                if 0 <= c < 2:

                    @pl.when(place[way] == n)
                    def _():
                        hop(way, c).wait_recv()
                        hop(way, c).start()


    chain(0)
    chain(1)
    for s in st:
        s.wait_recv()
    compact = compact + stats[1] + stats[2] + stats[3]
    stats[4] = compact
    st = [
        send(stats.at[4], stats.at[5], y_right),
        send(stats.at[4], stats.at[6], y_left),
        send(stats.at[4], stats.at[7], y_opp),
    ]
    relay(OWN, 0)
    relay(OWN, 1)
    offer_far(0)
    relay(OWN, 2)
    relay(OWN, 3)
    for s in st:
        s.wait_recv()
    compact = compact + stats[5] + stats[6] + stats[7]
    average = compact / D
    mean_below = pltpu.roll(average, 4, axis=0)
    spread = average - mean_below * mean_below
    both = jnp.where(rows < 4, average, lax.rsqrt(spread + EPS))
    columns[...] = jnp.transpose(jnp.concatenate([both] * 16, axis=0))

    def normalize(slot, groups=range(4)):
        gb = slabs[slot, :GB, :].astype(F32)
        gain, bias = gb[0:1], gb[8:9]
        for j in groups:
            x = slabs[slot, GB + j * 128 : GB + (j + 1) * 128, :].astype(F32)
            mean, rstd = columns[:, j : j + 1], columns[:, 4 + j : 5 + j]
            normed[j * 128 : (j + 1) * 128, (slot % 2) * FEAT : (slot % 2 + 1) * FEAT] = (
                (x - mean) * rstd * gain + bias
            ).astype(BF16)

    def project(pair, k, rows=slice(0, TOK)):
        product = dot(normed[rows], w_vm[pair, k])
        acc[k, rows] = product if pair == 0 else acc[k, rows] + product

    def weights_in(pair):
        for slot in (2 * pair, 2 * pair + 1):
            for c in w_loads[slot]:
                c.wait()

    normalize(0)
    offer_far(1)
    for i in (1, 3):
        from_left[OWN][i].wait_recv()
    normalize(1)
    weights_in(0)
    for k in range(3):
        project(0, k)
    offer_far(2)
    relay(OTHER, 0)
    for i in (0, 2):
        from_right[OWN][i].wait_recv()
    normalize(2)
    for i in range(4):
        from_opp[OWN][i].wait_recv()
    normalize(3)
    relay(OTHER, 1)
    weights_in(1)
    for k in range(3):
        project(1, k)

    wo_loads = []
    y_dest = [at["y"], y_right["y"], y_left["y"], y_opp["y"]]
    for b in range(4):
        first = (at["zh"] * 4 + y_dest[b]) * FEAT
        for d in range(4):
            wo_loads.append(
                load(
                    wo_ref.at[pl.ds(head_of[d] * HD, HD), pl.ds(first, FEAT)],
                    wo_vm.at[b, pl.ds(d * HD, HD)],
                )
            )

    offer_far(3)
    relay(OTHER, 2)
    weights_in(2)
    weights_in(3)

    def kv_part(side, core, d, p):
        return kv.at[side, core, :, d, pl.ds(p * QUARTER, QUARTER)]

    z_kv, z_q = {}, {}
    right_in, left_in, opp_in, mate_in = {}, {}, {}, {}

    def to_mate(side, d, p):
        mate_in[side, d, p] = send(kv_part(side, 0, d, p), kv_part(side, 1, d, p), mate)

    def spread_own(d, p):
        left_in[d, p] = send(kv_part(0, 0, d, p), kv_part(1, 0, d, p), x_right)
        right_in[d, p] = send(kv_part(0, 0, d, p), kv_part(2, 0, d, p), x_left)
        to_mate(0, d, p)

    def pass_on(d, p):
        left_in[d, p].wait_recv()
        if (d + p) % 2 == 0:
            opp_in[d, p] = send(kv_part(1, 0, d, p), kv_part(3, 0, d, p), x_right)
        to_mate(1, d, p)
        right_in[d, p].wait_recv()
        if (d + p) % 2 == 1:
            opp_in[d, p] = send(kv_part(2, 0, d, p), kv_part(3, 0, d, p), x_left)
        to_mate(2, d, p)

    def z_arrived(d, p):
        z_kv[d, p].wait_recv()
        spread_own(d, p)

    for p in (0, 1):
        groups = (2 * p, 2 * p + 1)
        half_p = slice(p * HALF, (p + 1) * HALF)
        normalize(4, groups)
        from_left[OTHER][2 * p + 1].wait_recv()
        normalize(5, groups)
        for k in range(3):
            project(2, k, half_p)
        if p == 1:
            chain(4)
        from_right[OTHER][2 * p].wait_recv()
        normalize(6, groups)
        for i in groups:
            from_opp[OTHER][i].wait_recv()
        normalize(7, groups)
        if p == 0:
            chain(2)
            relay(OTHER, 3)
            chain(3)
        else:
            chain(5)
        keep_p = pl.ds(p * HALF + at["row"] * QUARTER, QUARTER)
        give_p = pl.ds(p * HALF + mate["row"] * QUARTER, QUARTER)
        rows_p = pl.ds(p * QUARTER, QUARTER)
        halves = {}
        for k in (1, 2, 0):
            project(3, k, half_p)
            halves[k] = send(acc.at[k, give_p], arrived.at[p, k], mate)
        for k in (1, 2, 0):
            halves[k].wait_recv()
            whole = acc[k, keep_p, :] + arrived[p, k]
            if k == 0:
                whole = whole * SCALE
            whole = whole.astype(BF16)
            for d in (1, 2, 3):
                outgoing[p, d - 1, k] = whole[:, d * HD : (d + 1) * HD]
            if k == 0:
                q_vm[0, rows_p] = whole[:, :HD]
                for d in (1, 2, 3):
                    z_q[d, p] = send(outgoing.at[p, d - 1, 0], q_vm.at[d, rows_p], z_fwd[d])
            else:
                kv[0, 0, k - 1, 0, rows_p] = whole[:, :HD]
            if k == 2:
                for d in (1, 2, 3):
                    z_kv[d, p] = send(
                        outgoing.at[p, d - 1, pl.ds(1, 2)], kv_part(0, 0, d, p), z_fwd[d]
                    )
                spread_own(0, p)

    z_arrived(1, 0)
    z_arrived(2, 0)
    pass_on(0, 0)
    z_arrived(3, 0)
    pass_on(0, 1)
    z_arrived(1, 1)
    pass_on(1, 0)
    z_arrived(2, 1)
    pass_on(2, 0)
    z_arrived(3, 1)
    chain(6)
    pass_on(3, 0)
    for p in (0, 1):
        for d in (1, 2, 3):
            z_q[d, p].wait_recv()
    chain(7)

    ones = jnp.ones((KEYS, HD), BF16)
    n_q = 4 * HALF

    def attend(slots, begin, size, first):
        at_q = pl.ds(begin, size)
        q = q_vm[begin // HALF : (begin + size) // HALF].reshape(size, HD)
        best = None if first else top[at_q, :]
        total = None if first else blended[at_q, :]
        steps = [(slot, i) for slot in slots for i in range(n_q // KEYS)]
        d_step = KEYS // HALF

        def piece(step, k):
            (side, core), i = step
            return kv[side, core, k, i * d_step : (i + 1) * d_step].reshape(KEYS, HD)

        def lanes(values):
            return [values[:, c : c + HD] for c in range(0, values.shape[1], HD)]

        scores = dot(q, piece(steps[0], 0), ((1,), (1,)))
        for n, step in enumerate(steps):
            following = None
            if n + 1 < len(steps):
                following = dot(q, piece(steps[n + 1], 0), ((1,), (1,)))
            parts = lanes(scores)
            high = parts[0]
            for part in parts[1:]:
                high = jnp.maximum(high, part)
            now = jnp.broadcast_to(jnp.max(high, axis=1, keepdims=True), (size, HD))
            if best is not None:
                now = jnp.maximum(best, now)
            weights = [jnp.exp2(part - now).astype(BF16) for part in parts]
            product = dot(
                jnp.concatenate(weights, axis=1),
                jnp.concatenate([piece(step, 1), ones], axis=1),
            )
            if best is None:
                total = product
            else:
                shrink = jnp.exp2(best - now)
                total = jnp.concatenate([part * shrink for part in lanes(total)], axis=1) + product
            best, scores = now, following
        blended[at_q, :] = total
        top[at_q, :] = best

    def mates_in(side):
        for d in range(4):
            for p in (0, 1):
                mate_in[side, d, p].wait_recv()

    attend([(0, 0)], 0, n_q, True)
    pass_on(1, 1)
    pass_on(2, 1)
    mates_in(0)
    attend([(0, 1)], 0, n_q, False)
    pass_on(3, 1)
    for way in (0, 1):

        @pl.when(place[way] == 0)
        def _():
            for c in range(2):
                hop(way, c).wait_recv()

    def quarter(way, device):
        return wo_far.at[pl.ds(8 * way + 2 * device["x"], 2)]

    wo_left = [send(quarter(way, at), quarter(way, at), x_right) for way in (0, 1)]
    wo_right = [send(quarter(way, at), quarter(way, at), x_left) for way in (1, 0)][::-1]
    attend([(1, 0), (2, 0)], 0, n_q, False)
    for side in (1, 2):
        mates_in(side)
    attend([(1, 1), (2, 1)], 0, n_q, False)
    for d in range(4):
        for p in (0, 1):
            opp_in[d, p].wait_recv()
            to_mate(3, d, p)
    mates_in(3)

    c_in, f_in = {}, {}
    for begin in (2 * HALF, 0):
        attend([(3, 0), (3, 1)], begin, 2 * HALF, False)
        for d in (begin // HALF + 1, begin // HALF):
            rows_d = slice(d * HALF, (d + 1) * HALF)
            value = (blended[rows_d, :HD] / blended[rows_d, HD:]).astype(BF16)
            ctx_out[d] = value
            f_in[d] = send(ctx_out.at[d], ctx.at[1, 0, d], far_back[d])
            if d == 0:
                ctx[0, 0, 0] = value
            else:
                c_in[d] = send(ctx_out.at[d], ctx.at[0, 0, d], z_back[d])
    wo_left[0].wait_recv()
    wo_opp = [send(quarter(0, x_left), quarter(0, x_left), x_right)]
    wo_right[1].wait_recv()
    wo_opp.append(send(quarter(1, x_right), quarter(1, x_right), x_left))
    m_in = [send(ctx.at[0, 0, 0], ctx.at[0, 1, 0], mate)]
    for d in (3, 2, 1):
        c_in[d].wait_recv()
        m_in.append(send(ctx.at[0, 0, d], ctx.at[0, 1, d], mate))
    for d in (3, 2, 1, 0):
        f_in[d].wait_recv()
        m_in.append(send(ctx.at[1, 0, d], ctx.at[1, 1, d], mate))
    for c in wo_loads:
        c.wait()
    for c in (wo_left[1], wo_right[0], *wo_opp):
        c.wait_recv()
    def product(y, j):
        near = jnp.concatenate([ctx[0, j, d] for d in range(4)], axis=1)
        away = jnp.concatenate([ctx[1, j, d] for d in range(4)], axis=1)
        away_w = jnp.concatenate(
            [wo_far[y_dest[y] * 4 + head_of[d]] for d in range(4)], axis=0
        )
        return dot(near, wo_vm[y]) + dot(away, away_w)

    out_in = {}

    def push(name, j, value, device):
        partial[name, j] = value.astype(BF16)
        out_in[name, j] = send(partial.at[name, j], landed.at[name, j], device)

    def got(name, j):
        out_in[name, j].wait_recv()
        return landed[name, j].astype(F32)

    push(OPP, 0, product(OPP, 0), y_right)
    push(LEFT, 0, product(LEFT, 0), y_left)
    for m in m_in:
        m.wait_recv()
    push(OPP, 1, product(OPP, 1), y_left)
    push(RIGHT, 1, product(RIGHT, 1), y_right)
    push(RIGHT, 0, product(RIGHT, 0) + got(OPP, 0), y_right)
    push(LEFT, 1, product(LEFT, 1) + got(OPP, 1), y_left)
    for j in (0, 1):
        total = product(HERE, j)
        order = (LEFT, RIGHT) if j == 0 else (RIGHT, LEFT)
        total = total + got(order[0], j) + got(order[1], j)
        core = at["row"] if j == 0 else mate["row"]
        for p in (0, 1):
            first = p * HALF + core * QUARTER
            piece = total[p * QUARTER : (p + 1) * QUARTER]
            own = slabs[0, pl.ds(GB + first, QUARTER), :].astype(F32)
            out_ref[pl.ds(first, QUARTER), :] = (piece + own).astype(BF16)
    for copy in copies:
        copy.wait_send()
    for way in (0, 1):
        for c in range(2):
            hop(way, c).wait_send()


def body(tokens, ln_gain, ln_bias, w_qkv, w_out):
    any_spec = pl.BlockSpec(memory_space=pl.ANY)
    vmem_spec = pl.BlockSpec(memory_space=pltpu.VMEM)
    return pl.pallas_call(
        kernel,
        out_shape=jax.ShapeDtypeStruct((TOK, FEAT), BF16),
        in_specs=[any_spec, vmem_spec, vmem_spec, any_spec, any_spec],
        out_specs=pl.BlockSpec(memory_space=pltpu.VMEM),
        scratch_shapes=[
            pltpu.VMEM((8, TOK + GB, FEAT), BF16),
            pltpu.VMEM((TOK, 2 * FEAT), BF16),
            pltpu.VMEM((4, 3, 2 * FEAT, 4 * HD), BF16),
            pltpu.VMEM((4, 4 * HD, FEAT), BF16),
            pltpu.VMEM((16, HD, FEAT), BF16),
            pltpu.VMEM((3, TOK, 4 * HD), F32),
            pltpu.VMEM((2, 3, QUARTER, 4 * HD), F32),
            pltpu.VMEM((8, 8, 128), F32),
            pltpu.VMEM((128, 128), F32),
            pltpu.VMEM((2, 3, 3, QUARTER, HD), BF16),
            pltpu.VMEM((4, HALF, HD), BF16),
            pltpu.VMEM((4, 2, 2, 4, HALF, HD), BF16),
            pltpu.VMEM((4 * HALF, 128), F32),
            pltpu.VMEM((4 * HALF, 2 * HD), F32),
            pltpu.VMEM((4, HALF, HD), BF16),
            pltpu.VMEM((2, 2, 4, HALF, HD), BF16),
            pltpu.VMEM((4, 2, HALF, FEAT), BF16),
            pltpu.VMEM((4, 2, HALF, FEAT), BF16),
            pltpu.SemaphoreType.DMA((N_COPIES,)),
            pltpu.SemaphoreType.DMA((N_COPIES,)),
            pltpu.SemaphoreType.DMA((49,)),
            pltpu.SemaphoreType.DMA((2, 2)),
            pltpu.SemaphoreType.DMA((2, 2)),
        ],
        compiler_params=pltpu.CompilerParams(
            collective_id=0, has_side_effects=True, vmem_limit_bytes=60 * 2**20
        ),
    )(tokens, ln_gain[None], ln_bias[None], w_qkv, w_out)


def solution(mesh):
    finer = Mesh(mesh.devices.reshape(4, 4, 2, 2, 4), AXES)
    seq, row_col, col = ("x", "zl"), ("row", "zh", "y"), ("zh", "y")
    in_specs = (P(seq, row_col), P(row_col), P(row_col), P(None, "row", col), P(col, "row"))
    return jax.shard_map(
        body, mesh=finer, in_specs=in_specs, out_specs=P(seq, row_col), check_vma=False
    )
```

```python
import math

import jax
import jax.numpy as jnp
from jax import lax
from jax.experimental import pallas as pl
from jax.experimental.pallas import tpu as pltpu
from jax.sharding import Mesh
from jax.sharding import PartitionSpec as P

AXES = ("x", "zl", "row", "zh", "y")
MESH = pl.DeviceIdType.MESH
F32, BF16 = jnp.float32, jnp.bfloat16
D = 6144
EPS = 0.25
HD = 128
TOK = 512
QUARTER = 128
HALF = 256
FEAT = 384
GB = 16
SCALE = math.log2(math.e) / math.sqrt(HD)
KEYS = 512
OWN, OTHER = 0, 1
HERE, RIGHT, LEFT, OPP = 0, 1, 2, 3
N_COPIES = 150


def dot(a, b, dims=((1,), (0,))):
    return lax.dot_general(a, b, (dims, ((), ())), preferred_element_type=F32)


def kernel(
    tok_ref,
    gain_ref,
    bias_ref,
    w_ref,
    wo_ref,
    out_ref,
    slabs,
    normed,
    w_vm,
    wo_vm,
    wo_far,
    acc,
    arrived,
    stats,
    columns,
    outgoing,
    q_vm,
    kv,
    top,
    blended,
    ctx_out,
    ctx,
    partial,
    landed,
    send_sems,
    recv_sems,
    load_sems,
    chain_send,
    chain_recv,
):
    at = {a: lax.axis_index(a) for a in AXES}
    sizes = dict(x=4, zl=4, row=2, zh=2, y=4)

    def shifted(**by):
        return {
            a: lax.rem(at[a] + (by[a] % sizes[a]), sizes[a]) if a in by else at[a] for a in AXES
        }

    mate = shifted(row=1)
    far = shifted(zh=1)
    far_mate = shifted(zh=1, row=1)
    y_right, y_left, y_opp = shifted(y=1), shifted(y=-1), shifted(y=2)
    x_right, x_left = shifted(x=1), shifted(x=-1)
    z_fwd = [None] + [shifted(zl=d) for d in (1, 2, 3)]
    z_back = [None] + [shifted(zl=-d) for d in (1, 2, 3)]
    far_back = [shifted(zh=1, zl=-d) for d in range(4)]
    copies = []

    def send(src, dst, device):
        i = len(copies)
        copy = pltpu.make_async_remote_copy(
            src_ref=src,
            dst_ref=dst,
            send_sem=send_sems.at[i],
            recv_sem=recv_sems.at[i],
            device_id=device,
            device_id_type=MESH,
        )
        copy.start()
        copies.append(copy)
        return copy

    loads = []

    def load(src, dst):
        copy = pltpu.make_async_copy(src, dst, load_sems.at[len(loads)])
        copy.start()
        loads.append(copy)
        return copy

    own_tok = load(tok_ref, slabs.at[0, pl.ds(GB, TOK)])
    slabs[0, :GB, :] = jnp.where(
        lax.broadcasted_iota(jnp.int32, (GB, FEAT), 0) < 8,
        jnp.broadcast_to(gain_ref[...].astype(F32), (GB, FEAT)),
        jnp.broadcast_to(bias_ref[...].astype(F32), (GB, FEAT)),
    ).astype(BF16)

    y_of = [at["y"], y_left["y"], y_right["y"], y_opp["y"]]
    head_of = [at["zl"]] + [z_fwd[d]["zl"] for d in (1, 2, 3)]
    w_loads = []
    for slot in range(8):
        zh = at["zh"] if slot < 4 else far["zh"]
        first = (zh * 4 + y_of[slot % 4]) * FEAT
        w_loads.append(
            [
                load(
                    w_ref.at[:, pl.ds(first, FEAT), pl.ds(head_of[d] * HD, HD)],
                    w_vm.at[slot // 2, :, pl.ds((slot % 2) * FEAT, FEAT), pl.ds(d * HD, HD)],
                )
                for d in range(4)
            ]
        )

    barrier = pltpu.get_barrier_semaphore()
    partners = [mate, far, far_mate, y_right, y_left, y_opp, x_right, x_left, *z_fwd[1:], *far_back[1:]]
    for p in partners:
        pl.semaphore_signal(barrier, inc=1, device_id=p, device_id_type=MESH)
    own_tok.wait()

    rows8 = lax.broadcasted_iota(jnp.int32, (8, FEAT), 0)
    pick_sum = (rows8 < 4).astype(F32).astype(BF16)
    pick_sq = (rows8 >= 4).astype(F32).astype(BF16)
    mine = slabs[0, GB:, :]
    squares = mine.astype(F32) * mine.astype(F32)
    high = squares.astype(BF16)
    low = (squares - high.astype(F32)).astype(BF16)
    wide = (
        dot(pick_sum, mine, ((1,), (1,)))
        + dot(pick_sq, high, ((1,), (1,)))
        + dot(pick_sq, low, ((1,), (1,)))
    )
    rows = lax.broadcasted_iota(jnp.int32, (8, 128), 0)
    compact = jnp.zeros((8, 128), F32)
    for j in range(4):
        compact = jnp.where(rows % 4 == j, wide[:, j * 128 : (j + 1) * 128], compact)
    stats[0] = compact
    pl.semaphore_wait(barrier, len(partners))
    st = [
        send(stats.at[0], stats.at[1], mate),
        send(stats.at[0], stats.at[2], far),
        send(stats.at[0], stats.at[3], far_mate),
    ]

    chunks = [pl.ds(0, GB + QUARTER)] + [pl.ds(GB + i * QUARTER, QUARTER) for i in (1, 2, 3)]

    def move(src_slot, dst_slot, chunk, device):
        return send(slabs.at[src_slot, chunks[chunk]], slabs.at[dst_slot, chunks[chunk]], device)

    from_left, from_right, from_opp = [{}, {}], [{}, {}], [{}, {}]

    def offer(z, i):
        from_left[z][i] = move(4 * z, 4 * z + 1, i, y_right)
        from_right[z][i] = move(4 * z, 4 * z + 2, i, y_left)

    def relay(z, i):
        if i % 2 == 0:
            from_left[z][i].wait_recv()
            from_opp[z][i] = move(4 * z + 1, 4 * z + 3, i, y_right)
        else:
            from_right[z][i].wait_recv()
            from_opp[z][i] = move(4 * z + 2, 4 * z + 3, i, y_left)

    z_in = []
    for i in range(4):
        z_in.append(move(0, 4, i, far))
        offer(OWN, i)

    def offer_far(i):
        z_in[i].wait_recv()
        offer(OTHER, i)

    def wo_copy(way, c, t, src, device):
        return pltpu.make_async_remote_copy(
            src_ref=src,
            dst_ref=wo_far.at[8 * way + 2 * at["x"] + c],
            send_sem=chain_send.at[way, c, t],
            recv_sem=chain_recv.at[way, c],
            device_id=device,
            device_id_type=MESH,
        )

    source = [at["zl"] == 0, at["zl"] == 3]
    reached = [[dict(far, zl=jnp.int32(n)) for n in targets] for targets in ((3, 1), (0, 2))]
    relays = [lax.rem(at["zl"], 2) == 1, lax.rem(at["zl"], 2) == 0]
    beside = [z_back[1], z_fwd[1]]

    def wo_relay_copy(way, c):
        return wo_copy(way, c, 0, wo_far.at[8 * way + 2 * at["x"] + c], beside[way])

    def wo_start():
        for way in (0, 1):

            @pl.when(source[way])
            def _():
                for c in (0, 1):
                    block = 8 * way + 2 * at["x"] + c
                    first = (far["zh"] * 4 + lax.div(block, 4)) * FEAT
                    src = wo_ref.at[pl.ds(lax.rem(block, 4) * HD, HD), pl.ds(first, FEAT)]
                    for n in (0, 1):
                        wo_copy(way, c, n, src, reached[way][n]).start()

    def wo_relay():
        for way in (0, 1):

            @pl.when(relays[way])
            def _():
                for c in (0, 1):
                    wo_relay_copy(way, c).wait_recv()
                    wo_relay_copy(way, c).start()

    def wo_arrived():
        for way in (0, 1):

            @pl.when(jnp.logical_not(relays[way]))
            def _():
                for c in (0, 1):
                    wo_relay_copy(way, c).wait_recv()

    def wo_sent():
        for way in (0, 1):

            @pl.when(source[way])
            def _():
                for c in (0, 1):
                    for n in (0, 1):
                        wo_copy(
                            way, c, n, wo_far.at[8 * way + 2 * at["x"] + c], reached[way][n]
                        ).wait_send()

            @pl.when(relays[way])
            def _():
                for c in (0, 1):
                    wo_relay_copy(way, c).wait_send()

    wo_start()
    for s in st:
        s.wait_recv()
    compact = compact + stats[1] + stats[2] + stats[3]
    stats[4] = compact
    st = [
        send(stats.at[4], stats.at[5], y_right),
        send(stats.at[4], stats.at[6], y_left),
        send(stats.at[4], stats.at[7], y_opp),
    ]
    relay(OWN, 0)
    relay(OWN, 1)
    offer_far(0)
    relay(OWN, 2)
    relay(OWN, 3)
    for s in st:
        s.wait_recv()
    compact = compact + stats[5] + stats[6] + stats[7]
    average = compact / D
    mean_below = pltpu.roll(average, 4, axis=0)
    spread = average - mean_below * mean_below
    both = jnp.where(rows < 4, average, lax.rsqrt(spread + EPS))
    columns[...] = jnp.transpose(jnp.concatenate([both] * 16, axis=0))

    def normalize(slot, groups=range(4)):
        gb = slabs[slot, :GB, :].astype(F32)
        gain, bias = gb[0:1], gb[8:9]
        for j in groups:
            x = slabs[slot, GB + j * 128 : GB + (j + 1) * 128, :].astype(F32)
            mean, rstd = columns[:, j : j + 1], columns[:, 4 + j : 5 + j]
            normed[j * 128 : (j + 1) * 128, (slot % 2) * FEAT : (slot % 2 + 1) * FEAT] = (
                (x - mean) * rstd * gain + bias
            ).astype(BF16)

    def project(pair, k, rows=slice(0, TOK)):
        product = dot(normed[rows], w_vm[pair, k])
        acc[k, rows] = product if pair == 0 else acc[k, rows] + product

    def weights_in(pair):
        for slot in (2 * pair, 2 * pair + 1):
            for c in w_loads[slot]:
                c.wait()

    normalize(0)
    offer_far(1)
    for i in (1, 3):
        from_left[OWN][i].wait_recv()
    normalize(1)
    weights_in(0)
    for k in range(3):
        project(0, k)
    offer_far(2)
    relay(OTHER, 0)
    for i in (0, 2):
        from_right[OWN][i].wait_recv()
    normalize(2)
    for i in range(4):
        from_opp[OWN][i].wait_recv()
    normalize(3)
    relay(OTHER, 1)
    weights_in(1)
    for k in range(3):
        project(1, k)

    wo_loads = []
    y_dest = [at["y"], y_right["y"], y_left["y"], y_opp["y"]]
    for b in range(4):
        first = (at["zh"] * 4 + y_dest[b]) * FEAT
        for d in range(4):
            wo_loads.append(
                load(
                    wo_ref.at[pl.ds(head_of[d] * HD, HD), pl.ds(first, FEAT)],
                    wo_vm.at[b, pl.ds(d * HD, HD)],
                )
            )

    offer_far(3)
    relay(OTHER, 2)
    weights_in(2)
    weights_in(3)

    def kv_part(side, core, d, p):
        return kv.at[side, core, :, d, pl.ds(p * QUARTER, QUARTER)]

    z_kv, z_q = {}, {}
    right_in, left_in, opp_in, mate_in = {}, {}, {}, {}

    def to_mate(side, d, p):
        mate_in[side, d, p] = send(kv_part(side, 0, d, p), kv_part(side, 1, d, p), mate)

    def spread_own(d, p):
        left_in[d, p] = send(kv_part(0, 0, d, p), kv_part(1, 0, d, p), x_right)
        right_in[d, p] = send(kv_part(0, 0, d, p), kv_part(2, 0, d, p), x_left)
        to_mate(0, d, p)

    def pass_on(d, p):
        left_in[d, p].wait_recv()
        if (d + p) % 2 == 0:
            opp_in[d, p] = send(kv_part(1, 0, d, p), kv_part(3, 0, d, p), x_right)
        to_mate(1, d, p)
        right_in[d, p].wait_recv()
        if (d + p) % 2 == 1:
            opp_in[d, p] = send(kv_part(2, 0, d, p), kv_part(3, 0, d, p), x_left)
        to_mate(2, d, p)

    def z_arrived(d, p):
        z_kv[d, p].wait_recv()
        spread_own(d, p)

    for p in (0, 1):
        groups = (2 * p, 2 * p + 1)
        half_p = slice(p * HALF, (p + 1) * HALF)
        normalize(4, groups)
        from_left[OTHER][2 * p + 1].wait_recv()
        normalize(5, groups)
        for k in range(3):
            project(2, k, half_p)
        from_right[OTHER][2 * p].wait_recv()
        normalize(6, groups)
        for i in groups:
            from_opp[OTHER][i].wait_recv()
        normalize(7, groups)
        if p == 0:
            relay(OTHER, 3)
        keep_p = pl.ds(p * HALF + at["row"] * QUARTER, QUARTER)
        give_p = pl.ds(p * HALF + mate["row"] * QUARTER, QUARTER)
        rows_p = pl.ds(p * QUARTER, QUARTER)
        halves = {}
        for k in (1, 2, 0):
            project(3, k, half_p)
            halves[k] = send(acc.at[k, give_p], arrived.at[p, k], mate)
        for k in (1, 2, 0):
            halves[k].wait_recv()
            whole = acc[k, keep_p, :] + arrived[p, k]
            if k == 0:
                whole = whole * SCALE
            whole = whole.astype(BF16)
            for d in (1, 2, 3):
                outgoing[p, d - 1, k] = whole[:, d * HD : (d + 1) * HD]
            if k == 0:
                q_vm[p, 0] = whole[:, :HD]
                for d in (1, 2, 3):
                    z_q[d, p] = send(outgoing.at[p, d - 1, 0], q_vm.at[p, d], z_fwd[d])
            else:
                kv[0, 0, k - 1, 0, rows_p] = whole[:, :HD]
            if k == 2:
                for d in (1, 2, 3):
                    z_kv[d, p] = send(
                        outgoing.at[p, d - 1, pl.ds(1, 2)], kv_part(0, 0, d, p), z_fwd[d]
                    )
                spread_own(0, p)
    wo_relay()

    z_arrived(1, 0)
    z_arrived(2, 0)
    pass_on(0, 0)
    z_arrived(3, 0)
    pass_on(0, 1)
    z_arrived(1, 1)
    pass_on(1, 0)
    z_arrived(2, 1)
    pass_on(2, 0)
    z_arrived(3, 1)
    pass_on(3, 0)
    for p in (0, 1):
        for d in (1, 2, 3):
            z_q[d, p].wait_recv()

    ones = jnp.ones((KEYS, HD), BF16)
    n_q = 4 * HALF

    def attend(slots, begin, size, first):
        at_q = pl.ds(begin, size)
        q = q_vm[begin // TOK : (begin + size) // TOK].reshape(size, HD)
        best = None if first else top[at_q, :]
        total = None if first else blended[at_q, :]
        steps = [(slot, i) for slot in slots for i in range(n_q // KEYS)]
        d_step = KEYS // HALF

        def piece(step, k):
            (side, core), i = step
            return kv[side, core, k, i * d_step : (i + 1) * d_step].reshape(KEYS, HD)

        def lanes(values):
            return [values[:, c : c + HD] for c in range(0, values.shape[1], HD)]

        scores = dot(q, piece(steps[0], 0), ((1,), (1,)))
        for n, step in enumerate(steps):
            following = None
            if n + 1 < len(steps):
                following = dot(q, piece(steps[n + 1], 0), ((1,), (1,)))
            parts = lanes(scores)
            high = parts[0]
            for part in parts[1:]:
                high = jnp.maximum(high, part)
            now = jnp.broadcast_to(jnp.max(high, axis=1, keepdims=True), (size, HD))
            if best is not None:
                now = jnp.maximum(best, now)
            weights = [jnp.exp2(part - now).astype(BF16) for part in parts]
            product = dot(
                jnp.concatenate(weights, axis=1),
                jnp.concatenate([piece(step, 1), ones], axis=1),
            )
            if best is None:
                total = product
            else:
                shrink = jnp.exp2(best - now)
                total = jnp.concatenate([part * shrink for part in lanes(total)], axis=1) + product
            best, scores = now, following
        blended[at_q, :] = total
        top[at_q, :] = best

    def mates_in(side):
        for d in range(4):
            for p in (0, 1):
                mate_in[side, d, p].wait_recv()

    attend([(0, 0)], 0, n_q, True)
    pass_on(1, 1)
    pass_on(2, 1)
    mates_in(0)
    attend([(0, 1)], 0, n_q, False)
    pass_on(3, 1)
    wo_arrived()

    def quarter(way, device):
        return wo_far.at[pl.ds(8 * way + 2 * device["x"], 2)]

    wo_left = [send(quarter(way, at), quarter(way, at), x_right) for way in (0, 1)]
    wo_right = [send(quarter(way, at), quarter(way, at), x_left) for way in (1, 0)][::-1]
    attend([(1, 0), (2, 0)], 0, n_q, False)
    for side in (1, 2):
        mates_in(side)
    attend([(1, 1), (2, 1)], 0, n_q, False)
    for d in range(4):
        for p in (0, 1):
            opp_in[d, p].wait_recv()
            to_mate(3, d, p)
    mates_in(3)

    c_in, f_in = {}, {}
    for p in (0, 1):
        attend([(3, 0), (3, 1)], p * TOK, TOK, False)
        for d in (1, 2, 3, 0):
            first = p * TOK + d * QUARTER
            rows_d = slice(first, first + QUARTER)
            value = (blended[rows_d, :HD] / blended[rows_d, HD:]).astype(BF16)
            ctx_out[p, d] = value
            f_in[p, d] = send(ctx_out.at[p, d], ctx.at[1, 0, p, d], far_back[d])
            if d == 0:
                ctx[0, 0, p, 0] = value
            else:
                c_in[p, d] = send(ctx_out.at[p, d], ctx.at[0, 0, p, d], z_back[d])
    wo_left[0].wait_recv()
    wo_opp = [send(quarter(0, x_left), quarter(0, x_left), x_right)]
    wo_right[1].wait_recv()
    wo_opp.append(send(quarter(1, x_right), quarter(1, x_right), x_left))

    def product(y, j, p):
        near = jnp.concatenate([ctx[0, j, p, d] for d in range(4)], axis=1)
        away = jnp.concatenate([ctx[1, j, p, d] for d in range(4)], axis=1)
        away_w = jnp.concatenate(
            [wo_far[y_dest[y] * 4 + head_of[d]] for d in range(4)], axis=0
        )
        return dot(near, wo_vm[y]) + dot(away, away_w)

    out_in = {}

    def push(name, j, p, value, device):
        partial[name, j, p] = value.astype(BF16)
        out_in[name, j, p] = send(partial.at[name, j, p], landed.at[name, j, p], device)

    def got(name, j, p):
        out_in[name, j, p].wait_recv()
        return landed[name, j, p].astype(F32)

    for p in (0, 1):
        m_in = []
        for d in (1, 2, 3):
            c_in[p, d].wait_recv()
        m_in.append(send(ctx.at[0, 0, p], ctx.at[0, 1, p], mate))
        for d in (1, 2, 3, 0):
            f_in[p, d].wait_recv()
        m_in.append(send(ctx.at[1, 0, p], ctx.at[1, 1, p], mate))
        if p == 0:
            for c in wo_loads:
                c.wait()
            for c in (wo_left[1], wo_right[0], *wo_opp):
                c.wait_recv()
        push(OPP, 0, p, product(OPP, 0, p), y_right)
        push(LEFT, 0, p, product(LEFT, 0, p), y_left)
        for m in m_in:
            m.wait_recv()
        push(OPP, 1, p, product(OPP, 1, p), y_left)
        push(RIGHT, 1, p, product(RIGHT, 1, p), y_right)
        push(RIGHT, 0, p, product(RIGHT, 0, p) + got(OPP, 0, p), y_right)
        push(LEFT, 1, p, product(LEFT, 1, p) + got(OPP, 1, p), y_left)
    for p in (0, 1):
        for j in (0, 1):
            total = product(HERE, j, p)
            order = (LEFT, RIGHT) if j == 0 else (RIGHT, LEFT)
            total = total + got(order[0], j, p) + got(order[1], j, p)
            core = at["row"] if j == 0 else mate["row"]
            first = p * HALF + core * QUARTER
            own = slabs[0, pl.ds(GB + first, QUARTER), :].astype(F32)
            out_ref[pl.ds(first, QUARTER), :] = (total + own).astype(BF16)
    for copy in copies:
        copy.wait_send()
    wo_sent()


def body(tokens, ln_gain, ln_bias, w_qkv, w_out):
    any_spec = pl.BlockSpec(memory_space=pl.ANY)
    vmem_spec = pl.BlockSpec(memory_space=pltpu.VMEM)
    return pl.pallas_call(
        kernel,
        out_shape=jax.ShapeDtypeStruct((TOK, FEAT), BF16),
        in_specs=[any_spec, vmem_spec, vmem_spec, any_spec, any_spec],
        out_specs=pl.BlockSpec(memory_space=pltpu.VMEM),
        scratch_shapes=[
            pltpu.VMEM((8, TOK + GB, FEAT), BF16),
            pltpu.VMEM((TOK, 2 * FEAT), BF16),
            pltpu.VMEM((4, 3, 2 * FEAT, 4 * HD), BF16),
            pltpu.VMEM((4, 4 * HD, FEAT), BF16),
            pltpu.VMEM((16, HD, FEAT), BF16),
            pltpu.VMEM((3, TOK, 4 * HD), F32),
            pltpu.VMEM((2, 3, QUARTER, 4 * HD), F32),
            pltpu.VMEM((8, 8, 128), F32),
            pltpu.VMEM((128, 128), F32),
            pltpu.VMEM((2, 3, 3, QUARTER, HD), BF16),
            pltpu.VMEM((2, 4, QUARTER, HD), BF16),
            pltpu.VMEM((4, 2, 2, 4, HALF, HD), BF16),
            pltpu.VMEM((4 * HALF, 128), F32),
            pltpu.VMEM((4 * HALF, 2 * HD), F32),
            pltpu.VMEM((2, 4, QUARTER, HD), BF16),
            pltpu.VMEM((2, 2, 2, 4, QUARTER, HD), BF16),
            pltpu.VMEM((4, 2, 2, QUARTER, FEAT), BF16),
            pltpu.VMEM((4, 2, 2, QUARTER, FEAT), BF16),
            pltpu.SemaphoreType.DMA((N_COPIES,)),
            pltpu.SemaphoreType.DMA((N_COPIES,)),
            pltpu.SemaphoreType.DMA((49,)),
            pltpu.SemaphoreType.DMA((2, 2, 2)),
            pltpu.SemaphoreType.DMA((2, 2)),
        ],
        compiler_params=pltpu.CompilerParams(
            collective_id=0, has_side_effects=True, vmem_limit_bytes=60 * 2**20
        ),
    )(tokens, ln_gain[None], ln_bias[None], w_qkv, w_out)


def solution(mesh):
    finer = Mesh(mesh.devices.reshape(4, 4, 2, 2, 4), AXES)
    seq, row_col, col = ("x", "zl"), ("row", "zh", "y"), ("zh", "y")
    in_specs = (P(seq, row_col), P(row_col), P(row_col), P(None, "row", col), P(col, "row"))
    return jax.shard_map(
        body, mesh=finer, in_specs=in_specs, out_specs=P(seq, row_col), check_vma=False
    )
```

```python
import math

import jax
import jax.numpy as jnp
from jax import lax
from jax.experimental import pallas as pl
from jax.experimental.pallas import tpu as pltpu
from jax.sharding import Mesh
from jax.sharding import PartitionSpec as P

AXES = ("x", "zl", "row", "zh", "y")
MESH = pl.DeviceIdType.MESH
F32, BF16 = jnp.float32, jnp.bfloat16
D = 6144
EPS = 0.25
HD = 128
TOK = 512
QUARTER = 128
HALF = 256
FEAT = 384
GB = 16
SCALE = math.log2(math.e) / math.sqrt(HD)
KEYS = 512
OWN, OTHER = 0, 1
HERE, RIGHT, LEFT, OPP = 0, 1, 2, 3
N_COPIES = 150


def dot(a, b, dims=((1,), (0,))):
    return lax.dot_general(a, b, (dims, ((), ())), preferred_element_type=F32)


def kernel(
    tok_ref,
    scales_ref,
    w_ref,
    wo_ref,
    out_ref,
    slabs,
    normed,
    w_vm,
    wo_vm,
    wo_far,
    acc,
    arrived,
    stats,
    columns,
    outgoing,
    q_vm,
    kv,
    top,
    blended,
    ctx_out,
    ctx,
    partial,
    landed,
    send_sems,
    recv_sems,
    load_sems,
    chain_send,
    chain_recv,
):
    at = {a: lax.axis_index(a) for a in AXES}
    sizes = dict(x=4, zl=4, row=2, zh=2, y=4)

    def shifted(**by):
        return {
            a: lax.rem(at[a] + (by[a] % sizes[a]), sizes[a]) if a in by else at[a] for a in AXES
        }

    mate = shifted(row=1)
    far = shifted(zh=1)
    far_mate = shifted(zh=1, row=1)
    y_right, y_left, y_opp = shifted(y=1), shifted(y=-1), shifted(y=2)
    x_right, x_left = shifted(x=1), shifted(x=-1)
    z_fwd = [None] + [shifted(zl=d) for d in (1, 2, 3)]
    z_back = [None] + [shifted(zl=-d) for d in (1, 2, 3)]
    far_back = [shifted(zh=1, zl=-d) for d in range(4)]
    copies = []

    def send(src, dst, device):
        i = len(copies)
        copy = pltpu.make_async_remote_copy(
            src_ref=src,
            dst_ref=dst,
            send_sem=send_sems.at[i],
            recv_sem=recv_sems.at[i],
            device_id=device,
            device_id_type=MESH,
        )
        copy.start()
        copies.append(copy)
        return copy

    loads = []

    def load(src, dst):
        copy = pltpu.make_async_copy(src, dst, load_sems.at[len(loads)])
        copy.start()
        loads.append(copy)
        return copy

    own_tok = load(tok_ref, slabs.at[0, pl.ds(GB, TOK)])
    slabs[0, :GB, :] = jnp.where(
        lax.broadcasted_iota(jnp.int32, (GB, FEAT), 0) < 8,
        jnp.broadcast_to(scales_ref[0:1].astype(F32), (GB, FEAT)),
        jnp.broadcast_to(scales_ref[1:2].astype(F32), (GB, FEAT)),
    ).astype(BF16)

    y_of = [at["y"], y_left["y"], y_right["y"], y_opp["y"]]
    head_of = [at["zl"]] + [z_fwd[d]["zl"] for d in (1, 2, 3)]
    w_loads = []
    for slot in range(8):
        zh = at["zh"] if slot < 4 else far["zh"]
        first = (zh * 4 + y_of[slot % 4]) * FEAT
        w_loads.append(
            [
                load(
                    w_ref.at[:, pl.ds(first, FEAT), pl.ds(head_of[d] * HD, HD)],
                    w_vm.at[slot // 2, :, pl.ds((slot % 2) * FEAT, FEAT), pl.ds(d * HD, HD)],
                )
                for d in range(4)
            ]
        )

    barrier = pltpu.get_barrier_semaphore()
    partners = [mate, far, far_mate, y_right, y_left, y_opp, x_right, x_left, *z_fwd[1:], *far_back[1:]]
    for p in partners:
        pl.semaphore_signal(barrier, inc=1, device_id=p, device_id_type=MESH)
    own_tok.wait()

    rows8 = lax.broadcasted_iota(jnp.int32, (8, FEAT), 0)
    pick_sum = (rows8 < 4).astype(F32).astype(BF16)
    pick_sq = (rows8 >= 4).astype(F32).astype(BF16)
    mine = slabs[0, GB:, :]
    squares = mine.astype(F32) * mine.astype(F32)
    high = squares.astype(BF16)
    low = (squares - high.astype(F32)).astype(BF16)
    wide = (
        dot(pick_sum, mine, ((1,), (1,)))
        + dot(pick_sq, high, ((1,), (1,)))
        + dot(pick_sq, low, ((1,), (1,)))
    )
    rows = lax.broadcasted_iota(jnp.int32, (8, 128), 0)
    compact = jnp.zeros((8, 128), F32)
    for j in range(4):
        compact = jnp.where(rows % 4 == j, wide[:, j * 128 : (j + 1) * 128], compact)
    stats[0] = compact
    pl.semaphore_wait(barrier, len(partners))
    st = [
        send(stats.at[0], stats.at[1], mate),
        send(stats.at[0], stats.at[2], far),
        send(stats.at[0], stats.at[3], far_mate),
    ]

    chunks = [pl.ds(0, GB + QUARTER)] + [pl.ds(GB + i * QUARTER, QUARTER) for i in (1, 2, 3)]

    def move(src_slot, dst_slot, chunk, device):
        return send(slabs.at[src_slot, chunks[chunk]], slabs.at[dst_slot, chunks[chunk]], device)

    from_left, from_right, from_opp = [{}, {}], [{}, {}], [{}, {}]

    def offer(z, i):
        from_left[z][i] = move(4 * z, 4 * z + 1, i, y_right)
        from_right[z][i] = move(4 * z, 4 * z + 2, i, y_left)

    def relay(z, i):
        if i % 2 == 0:
            from_left[z][i].wait_recv()
            from_opp[z][i] = move(4 * z + 1, 4 * z + 3, i, y_right)
        else:
            from_right[z][i].wait_recv()
            from_opp[z][i] = move(4 * z + 2, 4 * z + 3, i, y_left)

    z_in = []
    for i in range(4):
        z_in.append(move(0, 4, i, far))
        offer(OWN, i)

    def offer_far(i):
        z_in[i].wait_recv()
        offer(OTHER, i)

    def wo_copy(way, c, t, src, device):
        return pltpu.make_async_remote_copy(
            src_ref=src,
            dst_ref=wo_far.at[8 * way + 2 * at["x"] + c],
            send_sem=chain_send.at[way, c, t],
            recv_sem=chain_recv.at[way, c],
            device_id=device,
            device_id_type=MESH,
        )

    source = [at["zl"] == 0, at["zl"] == 3]
    reached = [[dict(far, zl=jnp.int32(n)) for n in targets] for targets in ((3, 1), (0, 2))]
    relays = [lax.rem(at["zl"], 2) == 1, lax.rem(at["zl"], 2) == 0]
    beside = [z_back[1], z_fwd[1]]

    def wo_relay_copy(way, c):
        return wo_copy(way, c, 0, wo_far.at[8 * way + 2 * at["x"] + c], beside[way])

    def wo_start():
        for way in (0, 1):

            @pl.when(source[way])
            def _():
                for c in (0, 1):
                    block = 8 * way + 2 * at["x"] + c
                    first = (far["zh"] * 4 + lax.div(block, 4)) * FEAT
                    src = wo_ref.at[pl.ds(lax.rem(block, 4) * HD, HD), pl.ds(first, FEAT)]
                    for n in (0, 1):
                        wo_copy(way, c, n, src, reached[way][n]).start()

    def wo_relay():
        for way in (0, 1):

            @pl.when(relays[way])
            def _():
                for c in (0, 1):
                    wo_relay_copy(way, c).wait_recv()
                    wo_relay_copy(way, c).start()

    def wo_arrived():
        for way in (0, 1):

            @pl.when(jnp.logical_not(relays[way]))
            def _():
                for c in (0, 1):
                    wo_relay_copy(way, c).wait_recv()

    def wo_sent():
        for way in (0, 1):

            @pl.when(source[way])
            def _():
                for c in (0, 1):
                    for n in (0, 1):
                        wo_copy(
                            way, c, n, wo_far.at[8 * way + 2 * at["x"] + c], reached[way][n]
                        ).wait_send()

            @pl.when(relays[way])
            def _():
                for c in (0, 1):
                    wo_relay_copy(way, c).wait_send()

    wo_start()
    for s in st:
        s.wait_recv()
    compact = compact + stats[1] + stats[2] + stats[3]
    stats[4] = compact
    st = [
        send(stats.at[4], stats.at[5], y_right),
        send(stats.at[4], stats.at[6], y_left),
        send(stats.at[4], stats.at[7], y_opp),
    ]
    relay(OWN, 0)
    relay(OWN, 1)
    offer_far(0)
    relay(OWN, 2)
    relay(OWN, 3)
    for s in st:
        s.wait_recv()
    compact = compact + stats[5] + stats[6] + stats[7]
    average = compact / D
    mean_below = pltpu.roll(average, 4, axis=0)
    spread = average - mean_below * mean_below
    both = jnp.where(rows < 4, average, lax.rsqrt(spread + EPS))
    columns[...] = jnp.transpose(jnp.concatenate([both] * 16, axis=0))

    def normalize(slot, groups=range(4)):
        gb = slabs[slot, :GB, :].astype(F32)
        gain, bias = gb[0:1], gb[8:9]
        for j in groups:
            x = slabs[slot, GB + j * 128 : GB + (j + 1) * 128, :].astype(F32)
            mean, rstd = columns[:, j : j + 1], columns[:, 4 + j : 5 + j]
            normed[j * 128 : (j + 1) * 128, (slot % 2) * FEAT : (slot % 2 + 1) * FEAT] = (
                (x - mean) * rstd * gain + bias
            ).astype(BF16)

    def project(pair, k, rows=slice(0, TOK)):
        product = dot(normed[rows], w_vm[pair, k])
        acc[k, rows] = product if pair == 0 else acc[k, rows] + product

    def weights_in(pair):
        for slot in (2 * pair, 2 * pair + 1):
            for c in w_loads[slot]:
                c.wait()

    normalize(0)
    offer_far(1)
    for i in (1, 3):
        from_left[OWN][i].wait_recv()
    normalize(1)
    weights_in(0)
    for k in range(3):
        project(0, k)
    offer_far(2)
    relay(OTHER, 0)
    for i in (0, 2):
        from_right[OWN][i].wait_recv()
    normalize(2)
    for i in range(4):
        from_opp[OWN][i].wait_recv()
    normalize(3)
    relay(OTHER, 1)
    weights_in(1)
    for k in range(3):
        project(1, k)

    wo_loads = []
    y_dest = [at["y"], y_right["y"], y_left["y"], y_opp["y"]]
    for b in range(4):
        first = (at["zh"] * 4 + y_dest[b]) * FEAT
        for d in range(4):
            wo_loads.append(
                load(
                    wo_ref.at[pl.ds(head_of[d] * HD, HD), pl.ds(first, FEAT)],
                    wo_vm.at[b, pl.ds(d * HD, HD)],
                )
            )

    offer_far(3)
    relay(OTHER, 2)
    weights_in(2)
    weights_in(3)

    def kv_part(side, core, d, p):
        return kv.at[side, core, :, d, pl.ds(p * QUARTER, QUARTER)]

    z_kv, z_q = {}, {}
    right_in, left_in, opp_in, mate_in = {}, {}, {}, {}

    def to_mate(side, d, p):
        mate_in[side, d, p] = send(kv_part(side, 0, d, p), kv_part(side, 1, d, p), mate)

    def spread_own(d, p):
        left_in[d, p] = send(kv_part(0, 0, d, p), kv_part(1, 0, d, p), x_right)
        right_in[d, p] = send(kv_part(0, 0, d, p), kv_part(2, 0, d, p), x_left)
        to_mate(0, d, p)

    def pass_on(d, p):
        left_in[d, p].wait_recv()
        if (d + p) % 2 == 0:
            opp_in[d, p] = send(kv_part(1, 0, d, p), kv_part(3, 0, d, p), x_right)
        to_mate(1, d, p)
        right_in[d, p].wait_recv()
        if (d + p) % 2 == 1:
            opp_in[d, p] = send(kv_part(2, 0, d, p), kv_part(3, 0, d, p), x_left)
        to_mate(2, d, p)

    def z_arrived(d, p):
        z_kv[d, p].wait_recv()
        spread_own(d, p)

    for p in (0, 1):
        groups = (2 * p, 2 * p + 1)
        half_p = slice(p * HALF, (p + 1) * HALF)
        normalize(4, groups)
        from_left[OTHER][2 * p + 1].wait_recv()
        normalize(5, groups)
        for k in range(3):
            project(2, k, half_p)
        from_right[OTHER][2 * p].wait_recv()
        normalize(6, groups)
        for i in groups:
            from_opp[OTHER][i].wait_recv()
        normalize(7, groups)
        keep_p = pl.ds(p * HALF + at["row"] * QUARTER, QUARTER)
        give_p = pl.ds(p * HALF + mate["row"] * QUARTER, QUARTER)
        rows_p = pl.ds(p * QUARTER, QUARTER)
        halves = {}
        for k in (1, 2, 0):
            project(3, k, half_p)
            halves[k] = send(acc.at[k, give_p], arrived.at[p, k], mate)
        if p == 0:
            relay(OTHER, 3)
        for k in (1, 2, 0):
            halves[k].wait_recv()
            whole = acc[k, keep_p, :] + arrived[p, k]
            if k == 0:
                whole = whole * SCALE
            whole = whole.astype(BF16)
            for d in (1, 2, 3):
                outgoing[p, d - 1, k] = whole[:, d * HD : (d + 1) * HD]
            if k == 0:
                q_vm[p, 0] = whole[:, :HD]
                for d in (1, 2, 3):
                    z_q[d, p] = send(outgoing.at[p, d - 1, 0], q_vm.at[p, d], z_fwd[d])
            else:
                kv[0, 0, k - 1, 0, rows_p] = whole[:, :HD]
            if k == 2:
                for d in (1, 2, 3):
                    z_kv[d, p] = send(
                        outgoing.at[p, d - 1, pl.ds(1, 2)], kv_part(0, 0, d, p), z_fwd[d]
                    )
                spread_own(0, p)
    wo_relay()

    z_arrived(1, 0)
    z_arrived(2, 0)
    pass_on(0, 0)
    z_arrived(3, 0)
    pass_on(0, 1)
    z_arrived(1, 1)
    pass_on(1, 0)
    z_arrived(2, 1)
    pass_on(2, 0)
    z_arrived(3, 1)
    pass_on(3, 0)
    for p in (0, 1):
        for d in (1, 2, 3):
            z_q[d, p].wait_recv()

    ones = jnp.ones((KEYS, HD), BF16)
    n_q = 4 * HALF

    def attend(slots, begin, size, first):
        at_q = pl.ds(begin, size)
        q = q_vm[begin // TOK : (begin + size) // TOK].reshape(size, HD)
        best = None if first else top[at_q, :]
        total = None if first else blended[at_q, :]
        steps = [(slot, i) for slot in slots for i in range(n_q // KEYS)]
        d_step = KEYS // HALF

        def piece(step, k):
            (side, core), i = step
            return kv[side, core, k, i * d_step : (i + 1) * d_step].reshape(KEYS, HD)

        def lanes(values):
            return [values[:, c : c + HD] for c in range(0, values.shape[1], HD)]

        scores = dot(q, piece(steps[0], 0), ((1,), (1,)))
        for n, step in enumerate(steps):
            following = None
            if n + 1 < len(steps):
                following = dot(q, piece(steps[n + 1], 0), ((1,), (1,)))
            parts = lanes(scores)
            high = parts[0]
            for part in parts[1:]:
                high = jnp.maximum(high, part)
            now = jnp.broadcast_to(jnp.max(high, axis=1, keepdims=True), (size, HD))
            if best is not None:
                now = jnp.maximum(best, now)
            weights = [jnp.exp2(part - now).astype(BF16) for part in parts]
            product = dot(
                jnp.concatenate(weights, axis=1),
                jnp.concatenate([piece(step, 1), ones], axis=1),
            )
            if best is None:
                total = product
            else:
                shrink = jnp.exp2(best - now)
                total = jnp.concatenate([part * shrink for part in lanes(total)], axis=1) + product
            best, scores = now, following
        blended[at_q, :] = total
        top[at_q, :] = best

    def mates_in(side):
        for d in range(4):
            for p in (0, 1):
                mate_in[side, d, p].wait_recv()

    attend([(0, 0)], 0, n_q, True)
    pass_on(1, 1)
    pass_on(2, 1)
    mates_in(0)
    attend([(0, 1)], 0, n_q, False)
    pass_on(3, 1)
    wo_arrived()

    def quarter(way, device):
        return wo_far.at[pl.ds(8 * way + 2 * device["x"], 2)]

    wo_left = [send(quarter(way, at), quarter(way, at), x_right) for way in (0, 1)]
    wo_right = [send(quarter(way, at), quarter(way, at), x_left) for way in (1, 0)][::-1]
    attend([(1, 0), (2, 0)], 0, n_q, False)
    for side in (1, 2):
        mates_in(side)
    attend([(1, 1), (2, 1)], 0, n_q, False)
    for d in range(4):
        for p in (0, 1):
            opp_in[d, p].wait_recv()
            to_mate(3, d, p)
    mates_in(3)

    c_in, f_in = {}, {}
    for p in (0, 1):
        attend([(3, 0), (3, 1)], p * TOK, TOK, False)
        for d in (1, 2, 3, 0):
            first = p * TOK + d * QUARTER
            rows_d = slice(first, first + QUARTER)
            value = (blended[rows_d, :HD] / blended[rows_d, HD:]).astype(BF16)
            ctx_out[p, d] = value
            f_in[p, d] = send(ctx_out.at[p, d], ctx.at[1, 0, p, d], far_back[d])
            if d == 0:
                ctx[0, 0, p, 0] = value
            else:
                c_in[p, d] = send(ctx_out.at[p, d], ctx.at[0, 0, p, d], z_back[d])
    wo_left[0].wait_recv()
    wo_opp = [send(quarter(0, x_left), quarter(0, x_left), x_right)]
    wo_right[1].wait_recv()
    wo_opp.append(send(quarter(1, x_right), quarter(1, x_right), x_left))

    def product(y, j, p):
        near = jnp.concatenate([ctx[0, j, p, d] for d in range(4)], axis=1)
        away = jnp.concatenate([ctx[1, j, p, d] for d in range(4)], axis=1)
        away_w = jnp.concatenate(
            [wo_far[y_dest[y] * 4 + head_of[d]] for d in range(4)], axis=0
        )
        return dot(near, wo_vm[y]) + dot(away, away_w)

    out_in = {}

    def push(name, j, p, value, device):
        partial[name, j, p] = value.astype(BF16)
        out_in[name, j, p] = send(partial.at[name, j, p], landed.at[name, j, p], device)

    def got(name, j, p):
        out_in[name, j, p].wait_recv()
        return landed[name, j, p].astype(F32)

    for p in (0, 1):
        m_in = []
        for d in (1, 2, 3):
            c_in[p, d].wait_recv()
        m_in.append(send(ctx.at[0, 0, p], ctx.at[0, 1, p], mate))
        for d in (1, 2, 3, 0):
            f_in[p, d].wait_recv()
        m_in.append(send(ctx.at[1, 0, p], ctx.at[1, 1, p], mate))
        if p == 0:
            for c in wo_loads:
                c.wait()
            for c in (wo_left[1], wo_right[0], *wo_opp):
                c.wait_recv()
        push(OPP, 0, p, product(OPP, 0, p), y_right)
        push(LEFT, 0, p, product(LEFT, 0, p), y_left)
        for m in m_in:
            m.wait_recv()
        push(OPP, 1, p, product(OPP, 1, p), y_left)
        push(RIGHT, 1, p, product(RIGHT, 1, p), y_right)
        push(RIGHT, 0, p, product(RIGHT, 0, p) + got(OPP, 0, p), y_right)
        push(LEFT, 1, p, product(LEFT, 1, p) + got(OPP, 1, p), y_left)
    for p in (0, 1):
        for j in (0, 1):
            total = product(HERE, j, p)
            order = (LEFT, RIGHT) if j == 0 else (RIGHT, LEFT)
            total = total + got(order[0], j, p) + got(order[1], j, p)
            core = at["row"] if j == 0 else mate["row"]
            first = p * HALF + core * QUARTER
            own = slabs[0, pl.ds(GB + first, QUARTER), :].astype(F32)
            out_ref[pl.ds(first, QUARTER), :] = (total + own).astype(BF16)
    for copy in copies:
        copy.wait_send()
    wo_sent()


def body(tokens, ln_gain, ln_bias, w_qkv, w_out):
    any_spec = pl.BlockSpec(memory_space=pl.ANY)
    vmem_spec = pl.BlockSpec(memory_space=pltpu.VMEM)
    return pl.pallas_call(
        kernel,
        out_shape=jax.ShapeDtypeStruct((TOK, FEAT), BF16),
        in_specs=[any_spec, vmem_spec, any_spec, any_spec],
        out_specs=pl.BlockSpec(memory_space=pltpu.VMEM),
        scratch_shapes=[
            pltpu.VMEM((8, TOK + GB, FEAT), BF16),
            pltpu.VMEM((TOK, 2 * FEAT), BF16),
            pltpu.VMEM((4, 3, 2 * FEAT, 4 * HD), BF16),
            pltpu.VMEM((4, 4 * HD, FEAT), BF16),
            pltpu.VMEM((16, HD, FEAT), BF16),
            pltpu.VMEM((3, TOK, 4 * HD), F32),
            pltpu.VMEM((2, 3, QUARTER, 4 * HD), F32),
            pltpu.VMEM((8, 8, 128), F32),
            pltpu.VMEM((128, 128), F32),
            pltpu.VMEM((2, 3, 3, QUARTER, HD), BF16),
            pltpu.VMEM((2, 4, QUARTER, HD), BF16),
            pltpu.VMEM((4, 2, 2, 4, HALF, HD), BF16),
            pltpu.VMEM((4 * HALF, 128), F32),
            pltpu.VMEM((4 * HALF, 2 * HD), F32),
            pltpu.VMEM((2, 4, QUARTER, HD), BF16),
            pltpu.VMEM((2, 2, 2, 4, QUARTER, HD), BF16),
            pltpu.VMEM((4, 2, 2, QUARTER, FEAT), BF16),
            pltpu.VMEM((4, 2, 2, QUARTER, FEAT), BF16),
            pltpu.SemaphoreType.DMA((N_COPIES,)),
            pltpu.SemaphoreType.DMA((N_COPIES,)),
            pltpu.SemaphoreType.DMA((49,)),
            pltpu.SemaphoreType.DMA((2, 2, 2)),
            pltpu.SemaphoreType.DMA((2, 2)),
        ],
        compiler_params=pltpu.CompilerParams(
            collective_id=0, has_side_effects=True, vmem_limit_bytes=60 * 2**20
        ),
    )(tokens, jnp.stack([ln_gain, ln_bias]), w_qkv, w_out)


def solution(mesh):
    finer = Mesh(mesh.devices.reshape(4, 4, 2, 2, 4), AXES)
    seq, row_col, col = ("x", "zl"), ("row", "zh", "y"), ("zh", "y")
    in_specs = (P(seq, row_col), P(row_col), P(row_col), P(None, "row", col), P(col, "row"))
    return jax.shard_map(
        body, mesh=finer, in_specs=in_specs, out_specs=P(seq, row_col), check_vma=False
    )
```
